32 devices in a mesh: qa: 16 (over z, x, core), qb: 2 (over y).
Axes of the slice: x: 2, y: 2, z: 4, core: 2. Of those that a mesh axis runs over, the one named last changes fastest.
Arguments:
- wave_parts: float32 [2, 256, 128, 128], P(None, ('qa', 'qb')), may hold values from -6 to 6
- level_table: float32 [256, 128, 128], P(('qa', 'qb')), may hold values from -2 to 2
- phase_angles: float32 [2, 128], replicated, may hold values from 0.3 to 1.2
Outputs:
- final_parts: float32 [2, 256, 128, 128], P(None, ('qa', 'qb'))
The draws below stay inside these ranges and needn't reach their ends.
All inputs are finite; a program needn't handle non-finite values.
Results may differ from the reference program's by a relative error of at most 0.0003.
Values sent between devices are 32-bit elements; how exact they have to be, the bound alone decides.
A program may use at most 64 MiB of HBM per device.

```python
import jax
import jax.numpy as jnp
from jax import lax

BLOCKS_DEV = 8
ROWS = 128
LANES = 128
BLOCKS = 256
LAYERS = 2
N_QA = 16
N_QB = 2


def shard_levels(stream_key, dims, cuts, low, top_value):
    def one(position, blocks):
        heights = jax.random.uniform(jax.random.fold_in(jax.random.fold_in(stream_key, 6), position), (blocks,), jnp.float32, low / len(cuts), top_value / len(cuts))
        return jnp.repeat(jnp.exp(heights), dims[position] // blocks).reshape((-1,) + (1,) * (len(dims) - position - 1))

    gain = one(*cuts[0])
    for cut in cuts[1:]:
        gain = gain * one(*cut)
    return gain


def bell_draw(key, dims, width, most, pieces=(), kind=jnp.bfloat16):
    level = shard_levels(key, dims, pieces, -0.22, 0.18) if pieces else 1.0
    result = jax.random.normal(key, dims, jnp.float32) * width * level
    return jnp.minimum(jnp.maximum(result, -most), most).astype(kind)


def setup_inputs(seed: int = 0) -> dict:
    seeds = jax.random.split(jax.random.key(seed), 4)
    wave_parts = bell_draw(seeds[0], (2, BLOCKS, ROWS, LANES), 1.0, 6.0, ((1, 32),), jnp.float32)
    level_table = jnp.clip(jax.random.uniform(seeds[1], (BLOCKS, ROWS, LANES), jnp.float32, -2.0, 2.0) * shard_levels(seeds[1], (BLOCKS, ROWS, LANES), ((0, 32),), -0.4, 0.0), -2.0, 2.0)
    phase_angles = jnp.clip(jax.random.uniform(seeds[2], (LAYERS, LANES), jnp.float32, 0.3, 1.2), 0.3, 1.2)
    return {"wave_parts": wave_parts, "level_table": level_table, "phase_angles": phase_angles}


def count_bits(values, count):
    places = jnp.arange(count.bit_length() - 1, dtype=jnp.int32)
    return jnp.sum((values[..., None] >> places) & 1, axis=-1)


def sign_table(count):
    rank = jnp.arange(count, dtype=jnp.int32)
    parity = count_bits(rank[:, None] & rank[None, :], count) % 2
    real_part = jnp.where(parity == 1, -1.0, 1.0).astype(jnp.float32) * (count ** -0.5)
    return real_part


def turn_dim(values, dim):
    real_part = sign_table(values.shape[dim])
    def times(table):
        moved = jnp.tensordot(values, table, axes=([dim], [0]), precision=lax.Precision.HIGHEST)
        return jnp.moveaxis(moved, -1, dim)
    return times(real_part)


def turn_phase(values, levels, angle):
    turn = angle * levels
    return jnp.stack([values[0] * jnp.cos(turn) + values[1] * jnp.sin(turn), values[1] * jnp.cos(turn) - values[0] * jnp.sin(turn)])


def reference(wave_parts, level_table, phase_angles):
    values = wave_parts
    for layer in range(LAYERS):
        values = turn_phase(values, level_table, phase_angles[layer])
        values = turn_dim(values, 3)
        values = turn_dim(values, 2)
        parts = values.reshape(2, N_QA, N_QB, BLOCKS_DEV, ROWS, LANES)
        parts = turn_dim(parts, 1)
        parts = turn_dim(parts, 2)
        parts = turn_dim(parts, 3)
        values = parts.reshape(values.shape)
    return values
```

```python
import functools

import jax
import jax.numpy as jnp
import numpy as np
from jax import lax
from jax.experimental import pallas as pl
from jax.experimental.pallas import tpu as pltpu
from jax.sharding import PartitionSpec as P

MESH = pl.DeviceIdType.MESH
TURN_MOST = 2.5


def fit_even(function, degree):
    top = TURN_MOST**2
    nodes = (np.cos(np.pi * (np.arange(64) + 0.5) / 64) + 1) * top / 2
    fit = np.polynomial.chebyshev.Chebyshev.fit(nodes, function(np.sqrt(nodes)), degree, domain=[0, top])
    return [float(c) for c in fit.convert(kind=np.polynomial.Polynomial).coef]


COS = fit_even(np.cos, 6)
SIN = fit_even(lambda t: np.sin(t) / t, 5)


def horner(coefs, u, scale):
    total = jnp.float32(coefs[-1] * scale)
    for c in coefs[-2::-1]:
        total = total * u + jnp.float32(c * scale)
    return total


def cos_sin(turn, scale):
    u = turn * turn
    return horner(COS, u, scale), turn * horner(SIN, u, scale)


def sign_table(count):
    both = lax.broadcasted_iota(jnp.int32, (count, count), 0) & lax.broadcasted_iota(jnp.int32, (count, count), 1)
    shift = 1
    while shift < count.bit_length():
        shift *= 2
    while shift > 1:
        shift //= 2
        both = both ^ (both >> shift)
    return (1 - 2 * (both & 1)).astype(jnp.float32).astype(jnp.bfloat16)


def mix_lead(x):
    n = x.shape[0]
    half = 1
    while half < n:
        y = x.reshape((n // (2 * half), 2, half) + x.shape[1:])
        x = jnp.stack([y[:, 0] + y[:, 1], y[:, 0] - y[:, 1]], axis=1).reshape(x.shape)
        half *= 2
    return x


def mix_list(parts):
    half = 1
    while half < len(parts):
        mixed = list(parts)
        for k in range(len(parts)):
            if not k & half:
                mixed[k], mixed[k + half] = parts[k] + parts[k + half], parts[k] - parts[k + half]
        parts = mixed
        half *= 2
    return parts


def dot(a, b):
    return jnp.dot(a, b, preferred_element_type=jnp.float32)


def halves(x):
    hi = x.astype(jnp.bfloat16)
    return hi, (x - hi.astype(jnp.float32)).astype(jnp.bfloat16)


def mix_rows_lanes(rows, lanes, x, y):
    hi, lo = halves(jnp.concatenate([x, y], axis=1))
    both = dot(rows, hi) + dot(rows, lo)
    width = x.shape[1]
    out = []
    for part in (both[:, :width], both[:, width:]):
        hi, lo = halves(part)
        out.append(dot(hi, lanes) + dot(lo, lanes))
    return out


def kernel(
    na, nb, scales, wave_hbm, level_hbm, angle_hbm, out_ref,
    wave, level, angle, rows_table, lanes_table, mixed, send0, got0, send1, got1, levels, cosine, sine,
    load_sem, own_sem, ssem, rsem, level_sem,
):
    n = na * nb
    cuts, _, _, step, lanes = send0.shape
    qa, qb = lax.axis_index("qa"), lax.axis_index("qb")
    me = qa * nb + qb
    group = 4

    def flips(q, count):
        found = [q]
        bit = 1
        while bit < count:
            change = bit - 2 * bit * lax.rem(q // bit, 2)
            found = found + [f + change for f in found]
            bit *= 2
        return found

    to_as, to_bs = flips(qa, na), flips(qb, nb)
    order = [(ka, kb) for ka in far_first(na) for kb in range(nb) if ka or kb]
    peers = [(to_as[ka], to_bs[kb], to_as[ka] * nb + to_bs[kb]) for ka, kb in order]

    load_wave = pltpu.make_async_copy(wave_hbm, wave, load_sem.at[0])
    load_level = pltpu.make_async_copy(level_hbm, level, load_sem.at[1])
    load_angle = pltpu.make_async_copy(angle_hbm, angle, load_sem.at[2])
    load_level.start()
    load_angle.start()
    load_wave.start()

    barrier = pltpu.get_barrier_semaphore()
    for to_a, to_b, _ in peers[::-1]:
        pl.semaphore_signal(barrier, inc=1, device_id=(to_a, to_b), device_id_type=MESH)

    load_level.wait()
    pl.semaphore_wait(barrier, n - 1)

    def exchange(source, target, own, sent, got):
        pltpu.make_async_copy(source.at[me], target.at[me], own).start()
        for to_a, to_b, to in peers:
            pltpu.make_async_remote_copy(
                src_ref=source.at[to], dst_ref=target.at[me], send_sem=sent, recv_sem=got,
                device_id=(to_a, to_b), device_id_type=MESH,
            ).start()

    def received(source, target, own, got):
        pltpu.make_async_copy(source.at[me], target.at[me], own).wait()
        rest = target.at[pl.ds(0, n - 1)]
        pltpu.make_async_copy(rest, rest, got).wait()

    def left(source, sent):
        rest = source.at[pl.ds(0, n - 1)]
        pltpu.make_async_copy(rest, rest, sent).wait()

    exchange(level, levels, level_sem.at[0], level_sem.at[1], level_sem.at[2])
    rows_table[...] = sign_table(n * step)
    lanes_table[...] = sign_table(lanes)
    load_angle.wait()
    load_wave.wait()

    first = angle[0:1, :]

    @pl.loop(0, cuts)
    def _(cut):
        held = pl.ds(pl.multiple_of(cut * step, step), step)
        c, s = cos_sin(first * level[:, held, :].reshape(n * step, lanes), scales[0])
        x = wave[0, :, held, :].reshape(n * step, lanes)
        y = wave[1, :, held, :].reshape(n * step, lanes)
        done = mix_rows_lanes(rows_table[...], lanes_table[...], x * c + y * s, y * c - x * s)
        for part in range(2):
            mixed[cut, part] = done[part].reshape(n, step, lanes)

    for part in range(2):

        @pl.loop(0, n // group)
        def _(i):
            ds = pl.ds(i * group, group)
            send0[:, ds, part] = mix_lead(mixed[:, part, ds])

    @pl.loop(0, cuts)
    def _(cut):
        exchange(send0.at[cut], got0.at[cut], own_sem.at[0, cut], ssem.at[0, cut], rsem.at[0, cut])

    received(level, levels, level_sem.at[0], level_sem.at[2])
    second = angle[1:2, :]

    @pl.loop(0, n)
    def _(d):
        c, s = cos_sin(second * levels[d], scales[1])
        cosine[d] = c
        sine[d] = s

    @pl.loop(0, cuts)
    def _(cut):
        received(send0.at[cut], got0.at[cut], own_sem.at[0, cut], rsem.at[0, cut])
        held = pl.ds(pl.multiple_of(cut * step, step), step)
        x, y = mix_lead(got0[cut, :, 0]), mix_lead(got0[cut, :, 1])
        c, s = cosine[:, held, :], sine[:, held, :]
        x, y = (x * c + y * s).reshape(n * step, lanes), (y * c - x * s).reshape(n * step, lanes)
        done = mix_rows_lanes(rows_table[...], lanes_table[...], x, y)
        for part in range(2):
            send1[cut, :, part] = done[part].reshape(n, step, lanes)
        exchange(send1.at[cut], got1.at[cut], own_sem.at[1, cut], ssem.at[1, cut], rsem.at[1, cut])

    few = min(8, step)
    for cut in range(cuts):
        received(send1.at[cut], got1.at[cut], own_sem.at[1, cut], rsem.at[1, cut])
        last = cut == cuts - 1

        for part in range(2):
            for row in range(0, step, few):
                done = mix_lead(got1[cut, :, part, row : row + few])
                if not last:
                    mixed[cut, part, :, row : row + few] = done
                    continue
                parts = [mixed[k, part, :, row : row + few] for k in range(cut)] + [done]
                for k, value in enumerate(mix_list(parts)):
                    out_ref[part, :, k * step + row : k * step + row + few, :] = value

    left(level, level_sem.at[1])

    @pl.loop(0, cuts)
    def _(cut):
        left(send0.at[cut], ssem.at[0, cut])
        left(send1.at[cut], ssem.at[1, cut])


def put_out(state_ref, out_hbm, sem):
    copy = pltpu.make_async_copy(state_ref, out_hbm, sem)
    copy.start()
    copy.wait()


def far_first(count):
    quarter = count // 4
    low = [*range(0, quarter, 2), *range(1, quarter, 2)]
    return [high * quarter + k for high in (2, 3, 1, 0) for k in low] if quarter else range(count - 1, -1, -1)


STEP = 16
SPACE = 40 * 2**20


def body(wave_parts, level_table, phase_angles):
    na, nb = lax.axis_size("qa"), lax.axis_size("qb")
    n = na * nb
    _, blocks, rows, lanes = wave_parts.shape
    piece = blocks * rows // n
    step = min(STEP, piece)
    cuts = piece // step
    bits = (n * blocks * rows * lanes).bit_length() - 1
    scales = (2.0 ** -(bits // 2), 2.0 ** -(bits - bits // 2))
    hbm = pl.BlockSpec(memory_space=pltpu.HBM)
    f32 = jnp.float32
    flat = (2, n, piece, lanes)
    state = pltpu.VMEM((cuts, n, 2, step, lanes), f32)
    table = pltpu.VMEM((n, piece, lanes), f32)
    result = pl.pallas_call(
        functools.partial(kernel, na, nb, scales),
        out_shape=pltpu.VMEM(flat, f32),
        in_specs=[hbm, hbm, hbm],
        out_specs=pl.BlockSpec(memory_space=pltpu.VMEM),
        scratch_shapes=[
            pltpu.VMEM(flat, f32),
            table,
            pltpu.VMEM(phase_angles.shape, f32),
            pltpu.VMEM((n * step, n * step), jnp.bfloat16),
            pltpu.VMEM((lanes, lanes), jnp.bfloat16),
            pltpu.VMEM((cuts, 2, n, step, lanes), f32),
            state, state, state, state, table, table, table,
            pltpu.SemaphoreType.DMA((3,)),
            pltpu.SemaphoreType.DMA((2, cuts)),
            pltpu.SemaphoreType.DMA((2, cuts)),
            pltpu.SemaphoreType.DMA((2, cuts)),
            pltpu.SemaphoreType.DMA((3,)),
        ],
        compiler_params=pltpu.CompilerParams(
            collective_id=0, has_side_effects=True, vmem_limit_bytes=SPACE
        ),
    )(*(
        pltpu.with_memory_space_constraint(x, pltpu.HBM)
        for x in (wave_parts.reshape(flat), level_table.reshape(n, piece, lanes), phase_angles)
    ))
    result = pl.pallas_call(
        put_out,
        out_shape=jax.ShapeDtypeStruct(flat, f32),
        in_specs=[pl.BlockSpec(memory_space=pltpu.VMEM)],
        out_specs=hbm,
        scratch_shapes=[pltpu.SemaphoreType.DMA],
        compiler_params=pltpu.CompilerParams(vmem_limit_bytes=4 * 2**20),
    )(result)
    return result.reshape(wave_parts.shape)


def solution(mesh):
    in_specs = (P(None, ("qa", "qb"), None, None), P(("qa", "qb"), None, None), P())
    out_specs = P(None, ("qa", "qb"), None, None)
    return jax.shard_map(body, mesh=mesh, in_specs=in_specs, out_specs=out_specs, check_vma=False)
```

```python
import functools

import jax
import jax.numpy as jnp
import numpy as np
from jax import lax
from jax.experimental import pallas as pl
from jax.experimental.pallas import tpu as pltpu
from jax.sharding import PartitionSpec as P

MESH = pl.DeviceIdType.MESH
TURN_MOST = 2.5


def fit_even(function, degree):
    top = TURN_MOST**2
    nodes = (np.cos(np.pi * (np.arange(64) + 0.5) / 64) + 1) * top / 2
    fit = np.polynomial.chebyshev.Chebyshev.fit(nodes, function(np.sqrt(nodes)), degree, domain=[0, top])
    return [float(c) for c in fit.convert(kind=np.polynomial.Polynomial).coef]


COS = fit_even(np.cos, 6)
SIN = fit_even(lambda t: np.sin(t) / t, 5)


def horner(coefs, u, scale):
    total = jnp.float32(coefs[-1] * scale)
    for c in coefs[-2::-1]:
        total = total * u + jnp.float32(c * scale)
    return total


def cos_sin(turn, scale):
    u = turn * turn
    return horner(COS, u, scale), turn * horner(SIN, u, scale)


def sign_table(count):
    both = lax.broadcasted_iota(jnp.int32, (count, count), 0) & lax.broadcasted_iota(jnp.int32, (count, count), 1)
    shift = 1
    while shift < count.bit_length():
        shift *= 2
    while shift > 1:
        shift //= 2
        both = both ^ (both >> shift)
    return (1 - 2 * (both & 1)).astype(jnp.float32).astype(jnp.bfloat16)


def mix_lead(x):
    n = x.shape[0]
    half = 1
    while half < n:
        y = x.reshape((n // (2 * half), 2, half) + x.shape[1:])
        x = jnp.stack([y[:, 0] + y[:, 1], y[:, 0] - y[:, 1]], axis=1).reshape(x.shape)
        half *= 2
    return x


def mix_list(parts):
    half = 1
    while half < len(parts):
        mixed = list(parts)
        for k in range(len(parts)):
            if not k & half:
                mixed[k], mixed[k + half] = parts[k] + parts[k + half], parts[k] - parts[k + half]
        parts = mixed
        half *= 2
    return parts


def dot(a, b):
    return jnp.dot(a, b, preferred_element_type=jnp.float32)


def halves(x):
    hi = x.astype(jnp.bfloat16)
    return hi, (x - hi.astype(jnp.float32)).astype(jnp.bfloat16)


def mix_rows_lanes(rows, lanes, x, y):
    hi, lo = halves(jnp.concatenate([x, y], axis=1))
    both = dot(rows, hi) + dot(rows, lo)
    width = x.shape[1]
    out = []
    for part in (both[:, :width], both[:, width:]):
        hi, lo = halves(part)
        out.append(dot(hi, lanes) + dot(lo, lanes))
    return out


def kernel(
    na, nb, scales, wave_hbm, level_hbm, angle_hbm, out_ref,
    wave, level, angle, rows_table, lanes_table, mixed, send0, got0, send1, got1, levels, cosine, sine,
    load_sem, own_sem, ssem, rsem, level_sem, greet_sem,
):
    n = na * nb
    cuts, _, _, step, lanes = send0.shape
    qa, qb = lax.axis_index("qa"), lax.axis_index("qb")
    me = qa * nb + qb
    group = 4

    def flips(q, count):
        found = [q]
        bit = 1
        while bit < count:
            change = bit - 2 * bit * lax.rem(q // bit, 2)
            found = found + [f + change for f in found]
            bit *= 2
        return found

    to_as, to_bs = flips(qa, na), flips(qb, nb)
    order = [(ka, kb) for ka in far_first(na) for kb in range(nb) if ka or kb]
    peers = [(to_as[ka], to_bs[kb], to_as[ka] * nb + to_bs[kb]) for ka, kb in order]

    load_wave = pltpu.make_async_copy(wave_hbm, wave, load_sem.at[0])
    load_level = pltpu.make_async_copy(level_hbm, level, load_sem.at[1])
    load_angle = pltpu.make_async_copy(angle_hbm, angle, load_sem.at[2])
    load_level.start()
    load_angle.start()
    load_wave.start()

    def exchange(source, target, own, sent, got):
        pltpu.make_async_copy(source.at[me], target.at[me], own).start()
        for to_a, to_b, to in peers:
            pltpu.make_async_remote_copy(
                src_ref=source.at[to], dst_ref=target.at[me], send_sem=sent, recv_sem=got,
                device_id=(to_a, to_b), device_id_type=MESH,
            ).start()

    def received(source, target, own, got):
        pltpu.make_async_copy(source.at[me], target.at[me], own).wait()
        rest = target.at[pl.ds(0, n - 1)]
        pltpu.make_async_copy(rest, rest, got).wait()

    def left(source, sent):
        rest = source.at[pl.ds(0, n - 1)]
        pltpu.make_async_copy(rest, rest, sent).wait()

    inner = min(na, 4)
    depth = na // inner
    z, low = qa // inner, lax.rem(qa, inner)
    to_low = flips(low, inner)

    def reach(hop, m, k):
        return abs(hop) + m // 2 + k.bit_count()

    offsets = [
        (hop, m, k)
        for hop in sorted(range(1 - depth, depth), key=lambda h: -abs(h))
        for m in range(inner)
        for k in range(nb)
        if hop or m or k
    ]
    furthest = max(reach(*offset) for offset in offsets)

    def each(chosen, act):
        for hop, m, k in chosen:
            there = z + hop
            found = functools.partial(act, there * inner + to_low[m], to_bs[k])
            if hop:
                pl.when((there >= 0) & (there < depth))(found)
            else:
                found()

    def greet(count, sem, chosen):
        each(chosen, lambda a, b: pl.semaphore_signal(sem, inc=1, device_id=(a, b), device_id_type=MESH))
        sides = jnp.where(z > 0, 1, 0) + jnp.where(z < depth - 1, 1, 0)
        pl.semaphore_wait(sem, count(False) + sides * count(True))

    def send_level(a, b):
        pltpu.make_async_remote_copy(
            src_ref=level.at[a * nb + b], dst_ref=levels.at[me], send_sem=level_sem.at[1], recv_sem=level_sem.at[2],
            device_id=(a, b), device_id_type=MESH,
        ).start()

    for stage in range(furthest):
        near = [o for o in offsets if reach(*o) <= 1 and (stage == 0 or reach(*o) == 1 and o[1] % 2 == 0)]

        def count(along, near=near):
            return sum(o[0] == 1 if along else o[0] == 0 for o in near)

        greet(count, pltpu.get_barrier_semaphore() if stage == 0 else greet_sem.at[stage - 1], near)
        if stage == 0:
            load_level.wait()
            pltpu.make_async_copy(level.at[me], levels.at[me], level_sem.at[0]).start()
        each([o for o in offsets if reach(*o) == stage + 1 or stage == 0 and reach(*o) == 0], send_level)

    rows_table[...] = sign_table(n * step)
    lanes_table[...] = sign_table(lanes)
    load_angle.wait()
    load_wave.wait()

    first = angle[0:1, :]

    @pl.loop(0, cuts)
    def _(cut):
        held = pl.ds(pl.multiple_of(cut * step, step), step)
        c, s = cos_sin(first * level[:, held, :].reshape(n * step, lanes), scales[0])
        x = wave[0, :, held, :].reshape(n * step, lanes)
        y = wave[1, :, held, :].reshape(n * step, lanes)
        done = mix_rows_lanes(rows_table[...], lanes_table[...], x * c + y * s, y * c - x * s)
        for part in range(2):
            mixed[cut, part] = done[part].reshape(n, step, lanes)

    for part in range(2):

        @pl.loop(0, n // group)
        def _(i):
            ds = pl.ds(i * group, group)
            send0[:, ds, part] = mix_lead(mixed[:, part, ds])

    @pl.loop(0, cuts)
    def _(cut):
        exchange(send0.at[cut], got0.at[cut], own_sem.at[0, cut], ssem.at[0, cut], rsem.at[0, cut])

    received(level, levels, level_sem.at[0], level_sem.at[2])
    second = angle[1:2, :]

    @pl.loop(0, n)
    def _(d):
        c, s = cos_sin(second * levels[d], scales[1])
        cosine[d] = c
        sine[d] = s

    @pl.loop(0, cuts)
    def _(cut):
        received(send0.at[cut], got0.at[cut], own_sem.at[0, cut], rsem.at[0, cut])
        held = pl.ds(pl.multiple_of(cut * step, step), step)
        x, y = mix_lead(got0[cut, :, 0]), mix_lead(got0[cut, :, 1])
        c, s = cosine[:, held, :], sine[:, held, :]
        x, y = (x * c + y * s).reshape(n * step, lanes), (y * c - x * s).reshape(n * step, lanes)
        done = mix_rows_lanes(rows_table[...], lanes_table[...], x, y)
        for part in range(2):
            send1[cut, :, part] = done[part].reshape(n, step, lanes)
        exchange(send1.at[cut], got1.at[cut], own_sem.at[1, cut], ssem.at[1, cut], rsem.at[1, cut])

    few = min(8, step)
    for cut in range(cuts):
        received(send1.at[cut], got1.at[cut], own_sem.at[1, cut], rsem.at[1, cut])
        last = cut == cuts - 1

        for part in range(2):
            for row in range(0, step, few):
                done = mix_lead(got1[cut, :, part, row : row + few])
                if not last:
                    mixed[cut, part, :, row : row + few] = done
                    continue
                parts = [mixed[k, part, :, row : row + few] for k in range(cut)] + [done]
                for k, value in enumerate(mix_list(parts)):
                    out_ref[part, :, k * step + row : k * step + row + few, :] = value

    left(level, level_sem.at[1])

    @pl.loop(0, cuts)
    def _(cut):
        left(send0.at[cut], ssem.at[0, cut])
        left(send1.at[cut], ssem.at[1, cut])


def put_out(state_ref, out_hbm, sem):
    copy = pltpu.make_async_copy(state_ref, out_hbm, sem)
    copy.start()
    copy.wait()


def far_first(count):
    quarter = count // 4
    low = [*range(0, quarter, 2), *range(1, quarter, 2)]
    return [high * quarter + k for high in (2, 3, 1, 0) for k in low] if quarter else range(count - 1, -1, -1)


STEP = 16
SPACE = 40 * 2**20


def body(wave_parts, level_table, phase_angles):
    na, nb = lax.axis_size("qa"), lax.axis_size("qb")
    n = na * nb
    _, blocks, rows, lanes = wave_parts.shape
    piece = blocks * rows // n
    step = min(STEP, piece)
    cuts = piece // step
    bits = (n * blocks * rows * lanes).bit_length() - 1
    scales = (2.0 ** -(bits // 2), 2.0 ** -(bits - bits // 2))
    hbm = pl.BlockSpec(memory_space=pltpu.HBM)
    f32 = jnp.float32
    flat = (2, n, piece, lanes)
    state = pltpu.VMEM((cuts, n, 2, step, lanes), f32)
    table = pltpu.VMEM((n, piece, lanes), f32)
    result = pl.pallas_call(
        functools.partial(kernel, na, nb, scales),
        out_shape=pltpu.VMEM(flat, f32),
        in_specs=[hbm, hbm, hbm],
        out_specs=pl.BlockSpec(memory_space=pltpu.VMEM),
        scratch_shapes=[
            pltpu.VMEM(flat, f32),
            table,
            pltpu.VMEM(phase_angles.shape, f32),
            pltpu.VMEM((n * step, n * step), jnp.bfloat16),
            pltpu.VMEM((lanes, lanes), jnp.bfloat16),
            pltpu.VMEM((cuts, 2, n, step, lanes), f32),
            state, state, state, state, table, table, table,
            pltpu.SemaphoreType.DMA((3,)),
            pltpu.SemaphoreType.DMA((2, cuts)),
            pltpu.SemaphoreType.DMA((2, cuts)),
            pltpu.SemaphoreType.DMA((2, cuts)),
            pltpu.SemaphoreType.DMA((3,)),
            pltpu.SemaphoreType.REGULAR((n.bit_length() + na,)),
        ],
        compiler_params=pltpu.CompilerParams(
            collective_id=0, has_side_effects=True, vmem_limit_bytes=SPACE
        ),
    )(*(
        pltpu.with_memory_space_constraint(x, pltpu.HBM)
        for x in (wave_parts.reshape(flat), level_table.reshape(n, piece, lanes), phase_angles)
    ))
    result = pl.pallas_call(
        put_out,
        out_shape=jax.ShapeDtypeStruct(flat, f32),
        in_specs=[pl.BlockSpec(memory_space=pltpu.VMEM)],
        out_specs=hbm,
        scratch_shapes=[pltpu.SemaphoreType.DMA],
        compiler_params=pltpu.CompilerParams(vmem_limit_bytes=4 * 2**20),
    )(result)
    return result.reshape(wave_parts.shape)


def solution(mesh):
    in_specs = (P(None, ("qa", "qb"), None, None), P(("qa", "qb"), None, None), P())
    out_specs = P(None, ("qa", "qb"), None, None)
    return jax.shard_map(body, mesh=mesh, in_specs=in_specs, out_specs=out_specs, check_vma=False)
```

```python
import functools

import jax
import jax.numpy as jnp
import numpy as np
from jax import lax
from jax.experimental import pallas as pl
from jax.experimental.pallas import tpu as pltpu
from jax.sharding import PartitionSpec as P

MESH = pl.DeviceIdType.MESH
TURN_MOST = 2.5


def fit_even(function, degree):
    top = TURN_MOST**2
    nodes = (np.cos(np.pi * (np.arange(64) + 0.5) / 64) + 1) * top / 2
    fit = np.polynomial.chebyshev.Chebyshev.fit(nodes, function(np.sqrt(nodes)), degree, domain=[0, top])
    return [float(c) for c in fit.convert(kind=np.polynomial.Polynomial).coef]


COS = fit_even(np.cos, 6)
SIN = fit_even(lambda t: np.sin(t) / t, 5)


def horner(coefs, u, scale):
    total = jnp.float32(coefs[-1] * scale)
    for c in coefs[-2::-1]:
        total = total * u + jnp.float32(c * scale)
    return total


def cos_sin(turn, scale):
    u = turn * turn
    return horner(COS, u, scale), turn * horner(SIN, u, scale)


def sign_table(count):
    both = lax.broadcasted_iota(jnp.int32, (count, count), 0) & lax.broadcasted_iota(jnp.int32, (count, count), 1)
    shift = 1
    while shift < count.bit_length():
        shift *= 2
    while shift > 1:
        shift //= 2
        both = both ^ (both >> shift)
    return (1 - 2 * (both & 1)).astype(jnp.float32).astype(jnp.bfloat16)


def mix_lead(x):
    n = x.shape[0]
    half = 1
    while half < n:
        y = x.reshape((n // (2 * half), 2, half) + x.shape[1:])
        x = jnp.stack([y[:, 0] + y[:, 1], y[:, 0] - y[:, 1]], axis=1).reshape(x.shape)
        half *= 2
    return x


def mix_list(parts):
    half = 1
    while half < len(parts):
        mixed = list(parts)
        for k in range(len(parts)):
            if not k & half:
                mixed[k], mixed[k + half] = parts[k] + parts[k + half], parts[k] - parts[k + half]
        parts = mixed
        half *= 2
    return parts


def dot(a, b):
    return jnp.dot(a, b, preferred_element_type=jnp.float32)


def halves(x):
    hi = x.astype(jnp.bfloat16)
    return hi, (x - hi.astype(jnp.float32)).astype(jnp.bfloat16)


def mix_rows_lanes(rows, lanes, x, y):
    hi, lo = halves(jnp.concatenate([x, y], axis=1))
    both = dot(rows, hi) + dot(rows, lo)
    width = x.shape[1]
    out = []
    for part in (both[:, :width], both[:, width:]):
        hi, lo = halves(part)
        out.append(dot(hi, lanes) + dot(lo, lanes))
    return out


def kernel(
    na, nb, scales, wave_hbm, level_hbm, angle_hbm, out_ref,
    wave, level, angle, rows_table, lanes_table, mixed, send0, got0, send1, got1, levels, cosine, sine,
    load_sem, own_sem, ssem, rsem, level_sem, greet_sem,
):
    n = na * nb
    cuts, _, _, step, lanes = send0.shape
    qa, qb = lax.axis_index("qa"), lax.axis_index("qb")
    me = qa * nb + qb
    group = 4

    def flips(q, count):
        found = [q]
        bit = 1
        while bit < count:
            change = bit - 2 * bit * lax.rem(q // bit, 2)
            found = found + [f + change for f in found]
            bit *= 2
        return found

    to_as, to_bs = flips(qa, na), flips(qb, nb)
    order = [(ka, kb) for ka in far_first(na) for kb in range(nb) if ka or kb]
    peers = [(to_as[ka], to_bs[kb], to_as[ka] * nb + to_bs[kb]) for ka, kb in order]

    load_wave = pltpu.make_async_copy(wave_hbm, wave, load_sem.at[0])
    load_level = pltpu.make_async_copy(level_hbm, level, load_sem.at[1])
    load_angle = pltpu.make_async_copy(angle_hbm, angle, load_sem.at[2])
    load_level.start()
    load_angle.start()
    load_wave.start()

    def exchange(source, target, own, sent, got):
        pltpu.make_async_copy(source.at[me], target.at[me], own).start()
        for to_a, to_b, to in peers:
            pltpu.make_async_remote_copy(
                src_ref=source.at[to], dst_ref=target.at[me], send_sem=sent, recv_sem=got,
                device_id=(to_a, to_b), device_id_type=MESH,
            ).start()

    def received(source, target, own, got):
        pltpu.make_async_copy(source.at[me], target.at[me], own).wait()
        rest = target.at[pl.ds(0, n - 1)]
        pltpu.make_async_copy(rest, rest, got).wait()

    def left(source, sent):
        rest = source.at[pl.ds(0, n - 1)]
        pltpu.make_async_copy(rest, rest, sent).wait()

    inner = min(na, 4)
    depth = na // inner
    z, core = qa // inner, lax.rem(qa, 2)
    steps = [("qa", 2)] * (inner == 4) + [("qb", 1 << k) for k in range(nb.bit_length() - 1)]
    sides = []
    for mask in range(1 << len(steps)):
        side_a, side_b, later = lax.rem(qa, inner), qb, jnp.int32(0)
        for k, (axis, bit) in enumerate(steps):
            if mask >> k & 1:
                there = lax.rem((qa if axis == "qa" else qb) // bit, 2)
                later += 1 - there
                side_a += (bit - 2 * bit * there) * (axis == "qa")
                side_b += (bit - 2 * bit * there) * (axis == "qb")
        sides.append((mask.bit_count(), later, side_a, side_b))

    def below(size, later):
        return later == 0

    def above(size, later):
        return later == size

    def tell(sem_of, low, high, chosen, both):
        for mask, (size, later, a, b) in enumerate(sides):
            for other in range(1 + both):

                @pl.when(chosen(size, later))
                def _():
                    skip = not mask and not other
                    bounds = (low + (skip and chosen is above), high - (skip and chosen is below))

                    def one(to_z, _):
                        to_a = to_z * inner + a + other * (1 - 2 * core)
                        pl.semaphore_signal(sem_of(size, to_z), inc=1, device_id=(to_a, b), device_id_type=MESH)

                    lax.fori_loop(*bounds, one, None)

    def send_levels(found):
        for mask, (_, later, a, b) in enumerate(sides):
            for other in range(2):
                ahead = z + found - later
                own_chip = 1 if not mask and not other else 0
                low = jnp.where(later < found, ahead, 0)
                high = jnp.where(later < found, jnp.minimum(ahead + 1, depth), jnp.where(later == found, z + 1 - own_chip, 0))

                def one(to_z, _):
                    to_a = to_z * inner + a + other * (1 - 2 * core)
                    pltpu.make_async_remote_copy(
                        src_ref=level.at[to_a * nb + b], dst_ref=levels.at[me],
                        send_sem=level_sem.at[1], recv_sem=level_sem.at[2],
                        device_id=(to_a, b), device_id_type=MESH,
                    ).start()

                lax.fori_loop(low, high, one, None)

    barrier = pltpu.get_barrier_semaphore()
    tell(lambda size, to_z: barrier, z, depth, above, True)
    nearer = sum(jnp.where(below(size, later), 1, 0) for size, later, _, _ in sides)
    pl.semaphore_wait(barrier, 2 * (z + 1) * nearer - 1)
    tell(lambda size, to_z: greet_sem.at[size + z - to_z - 1], 0, z + 1, below, False)
    load_level.wait()
    send_levels(0)
    pltpu.make_async_copy(level.at[me], levels.at[me], level_sem.at[0]).start()
    for found in range(1, len(steps) + depth):
        fresh = sum(
            jnp.where(above(size, later) & (found >= size) & (z + found - size < depth), 1, 0) for size, later, _, _ in sides
        )

        @pl.when(fresh > 0)
        def _():
            pl.semaphore_wait(greet_sem.at[found - 1], fresh)
            send_levels(found)

    rows_table[...] = sign_table(n * step)
    lanes_table[...] = sign_table(lanes)
    load_angle.wait()
    load_wave.wait()

    first = angle[0:1, :]

    @pl.loop(0, cuts)
    def _(cut):
        held = pl.ds(pl.multiple_of(cut * step, step), step)
        c, s = cos_sin(first * level[:, held, :].reshape(n * step, lanes), scales[0])
        x = wave[0, :, held, :].reshape(n * step, lanes)
        y = wave[1, :, held, :].reshape(n * step, lanes)
        done = mix_rows_lanes(rows_table[...], lanes_table[...], x * c + y * s, y * c - x * s)
        for part in range(2):
            mixed[cut, part] = done[part].reshape(n, step, lanes)

    for part in range(2):

        @pl.loop(0, n // group)
        def _(i):
            ds = pl.ds(i * group, group)
            send0[:, ds, part] = mix_lead(mixed[:, part, ds])

    @pl.loop(0, cuts)
    def _(cut):
        exchange(send0.at[cut], got0.at[cut], own_sem.at[0, cut], ssem.at[0, cut], rsem.at[0, cut])

    received(level, levels, level_sem.at[0], level_sem.at[2])
    second = angle[1:2, :]

    @pl.loop(0, n)
    def _(d):
        c, s = cos_sin(second * levels[d], scales[1])
        cosine[d] = c
        sine[d] = s

    @pl.loop(0, cuts)
    def _(cut):
        received(send0.at[cut], got0.at[cut], own_sem.at[0, cut], rsem.at[0, cut])
        held = pl.ds(pl.multiple_of(cut * step, step), step)
        x, y = mix_lead(got0[cut, :, 0]), mix_lead(got0[cut, :, 1])
        c, s = cosine[:, held, :], sine[:, held, :]
        x, y = (x * c + y * s).reshape(n * step, lanes), (y * c - x * s).reshape(n * step, lanes)
        done = mix_rows_lanes(rows_table[...], lanes_table[...], x, y)
        for part in range(2):
            send1[cut, :, part] = done[part].reshape(n, step, lanes)
        exchange(send1.at[cut], got1.at[cut], own_sem.at[1, cut], ssem.at[1, cut], rsem.at[1, cut])

    few = min(8, step)
    for cut in range(cuts):
        received(send1.at[cut], got1.at[cut], own_sem.at[1, cut], rsem.at[1, cut])
        last = cut == cuts - 1

        for part in range(2):
            for row in range(0, step, few):
                done = mix_lead(got1[cut, :, part, row : row + few])
                if not last:
                    mixed[cut, part, :, row : row + few] = done
                    continue
                parts = [mixed[k, part, :, row : row + few] for k in range(cut)] + [done]
                for k, value in enumerate(mix_list(parts)):
                    out_ref[part, :, k * step + row : k * step + row + few, :] = value

    left(level, level_sem.at[1])

    @pl.loop(0, cuts)
    def _(cut):
        left(send0.at[cut], ssem.at[0, cut])
        left(send1.at[cut], ssem.at[1, cut])


def put_out(state_ref, out_hbm, sem):
    copy = pltpu.make_async_copy(state_ref, out_hbm, sem)
    copy.start()
    copy.wait()


def far_first(count):
    quarter = count // 4
    low = [*range(0, quarter, 2), *range(1, quarter, 2)]
    return [high * quarter + k for high in (2, 3, 1, 0) for k in low] if quarter else range(count - 1, -1, -1)


STEP = 16
SPACE = 40 * 2**20


def body(wave_parts, level_table, phase_angles):
    na, nb = lax.axis_size("qa"), lax.axis_size("qb")
    n = na * nb
    _, blocks, rows, lanes = wave_parts.shape
    piece = blocks * rows // n
    step = min(STEP, piece)
    cuts = piece // step
    bits = (n * blocks * rows * lanes).bit_length() - 1
    scales = (2.0 ** -(bits // 2), 2.0 ** -(bits - bits // 2))
    hbm = pl.BlockSpec(memory_space=pltpu.HBM)
    f32 = jnp.float32
    flat = (2, n, piece, lanes)
    state = pltpu.VMEM((cuts, n, 2, step, lanes), f32)
    table = pltpu.VMEM((n, piece, lanes), f32)
    result = pl.pallas_call(
        functools.partial(kernel, na, nb, scales),
        out_shape=pltpu.VMEM(flat, f32),
        in_specs=[hbm, hbm, hbm],
        out_specs=pl.BlockSpec(memory_space=pltpu.VMEM),
        scratch_shapes=[
            pltpu.VMEM(flat, f32),
            table,
            pltpu.VMEM(phase_angles.shape, f32),
            pltpu.VMEM((n * step, n * step), jnp.bfloat16),
            pltpu.VMEM((lanes, lanes), jnp.bfloat16),
            pltpu.VMEM((cuts, 2, n, step, lanes), f32),
            state, state, state, state, table, table, table,
            pltpu.SemaphoreType.DMA((3,)),
            pltpu.SemaphoreType.DMA((2, cuts)),
            pltpu.SemaphoreType.DMA((2, cuts)),
            pltpu.SemaphoreType.DMA((2, cuts)),
            pltpu.SemaphoreType.DMA((3,)),
            pltpu.SemaphoreType.REGULAR((nb.bit_length() + na,)),
        ],
        compiler_params=pltpu.CompilerParams(
            collective_id=0, has_side_effects=True, vmem_limit_bytes=SPACE
        ),
    )(*(
        pltpu.with_memory_space_constraint(x, pltpu.HBM)
        for x in (wave_parts.reshape(flat), level_table.reshape(n, piece, lanes), phase_angles)
    ))
    result = pl.pallas_call(
        put_out,
        out_shape=jax.ShapeDtypeStruct(flat, f32),
        in_specs=[pl.BlockSpec(memory_space=pltpu.VMEM)],
        out_specs=hbm,
        scratch_shapes=[pltpu.SemaphoreType.DMA],
        compiler_params=pltpu.CompilerParams(vmem_limit_bytes=4 * 2**20),
    )(result)
    return result.reshape(wave_parts.shape)


def solution(mesh):
    in_specs = (P(None, ("qa", "qb"), None, None), P(("qa", "qb"), None, None), P())
    out_specs = P(None, ("qa", "qb"), None, None)
    return jax.shard_map(body, mesh=mesh, in_specs=in_specs, out_specs=out_specs, check_vma=False)
```

```python
import functools

import jax
import jax.numpy as jnp
import numpy as np
from jax import lax
from jax.experimental import pallas as pl
from jax.experimental.pallas import tpu as pltpu
from jax.sharding import PartitionSpec as P

MESH = pl.DeviceIdType.MESH
TURN_MOST = 2.5


def fit_even(function, degree):
    top = TURN_MOST**2
    nodes = (np.cos(np.pi * (np.arange(64) + 0.5) / 64) + 1) * top / 2
    fit = np.polynomial.chebyshev.Chebyshev.fit(nodes, function(np.sqrt(nodes)), degree, domain=[0, top])
    return [float(c) for c in fit.convert(kind=np.polynomial.Polynomial).coef]


COS = fit_even(np.cos, 6)
SIN = fit_even(lambda t: np.sin(t) / t, 5)


def horner(coefs, u, scale):
    total = jnp.float32(coefs[-1] * scale)
    for c in coefs[-2::-1]:
        total = total * u + jnp.float32(c * scale)
    return total


def cos_sin(turn, scale):
    u = turn * turn
    return horner(COS, u, scale), turn * horner(SIN, u, scale)


def sign_table(count):
    both = lax.broadcasted_iota(jnp.int32, (count, count), 0) & lax.broadcasted_iota(jnp.int32, (count, count), 1)
    shift = 1
    while shift < count.bit_length():
        shift *= 2
    while shift > 1:
        shift //= 2
        both = both ^ (both >> shift)
    return (1 - 2 * (both & 1)).astype(jnp.float32).astype(jnp.bfloat16)


def mix_lead(x):
    n = x.shape[0]
    half = 1
    while half < n:
        y = x.reshape((n // (2 * half), 2, half) + x.shape[1:])
        x = jnp.stack([y[:, 0] + y[:, 1], y[:, 0] - y[:, 1]], axis=1).reshape(x.shape)
        half *= 2
    return x


def mix_list(parts):
    half = 1
    while half < len(parts):
        mixed = list(parts)
        for k in range(len(parts)):
            if not k & half:
                mixed[k], mixed[k + half] = parts[k] + parts[k + half], parts[k] - parts[k + half]
        parts = mixed
        half *= 2
    return parts


def dot(a, b):
    return jnp.dot(a, b, preferred_element_type=jnp.float32)


def halves(x):
    hi = x.astype(jnp.bfloat16)
    return hi, (x - hi.astype(jnp.float32)).astype(jnp.bfloat16)


def mix_rows_lanes(rows, lanes, x, y):
    hi, lo = halves(jnp.concatenate([x, y], axis=1))
    both = dot(rows, hi) + dot(rows, lo)
    width = x.shape[1]
    out = []
    for part in (both[:, :width], both[:, width:]):
        hi, lo = halves(part)
        out.append(dot(hi, lanes) + dot(lo, lanes))
    return out


def kernel(
    na, nb, scales, wave_hbm, level_hbm, angle_hbm, out_ref,
    wave, level, angle, rows_table, lanes_table, mixed, send0, got0, send1, got1, levels, cosine, sine,
    load_sem, own_sem, ssem, rsem, level_sem, greet_sem,
):
    n = na * nb
    cuts, _, _, step, lanes = send0.shape
    qa, qb = lax.axis_index("qa"), lax.axis_index("qb")
    me = qa * nb + qb
    group = 4

    def flips(q, count):
        found = [q]
        bit = 1
        while bit < count:
            change = bit - 2 * bit * lax.rem(q // bit, 2)
            found = found + [f + change for f in found]
            bit *= 2
        return found

    to_as, to_bs = flips(qa, na), flips(qb, nb)
    order = far_first(na, nb)
    peers = [(to_as[ka], to_bs[kb], to_as[ka] * nb + to_bs[kb]) for ka, kb in order]

    load_wave = pltpu.make_async_copy(wave_hbm, wave, load_sem.at[0])
    load_level = pltpu.make_async_copy(level_hbm, level, load_sem.at[1])
    load_angle = pltpu.make_async_copy(angle_hbm, angle, load_sem.at[2])
    load_level.start()
    load_angle.start()
    load_wave.start()

    def exchange(source, target, own, sent, got):
        pltpu.make_async_copy(source.at[me], target.at[me], own).start()
        for to_a, to_b, to in peers:
            pltpu.make_async_remote_copy(
                src_ref=source.at[to], dst_ref=target.at[me], send_sem=sent, recv_sem=got,
                device_id=(to_a, to_b), device_id_type=MESH,
            ).start()

    def received(source, target, own, got):
        pltpu.make_async_copy(source.at[me], target.at[me], own).wait()
        rest = target.at[pl.ds(0, n - 1)]
        pltpu.make_async_copy(rest, rest, got).wait()

    def left(source, sent):
        rest = source.at[pl.ds(0, n - 1)]
        pltpu.make_async_copy(rest, rest, sent).wait()

    inner = min(na, 4)
    depth = na // inner
    z, core = qa // inner, lax.rem(qa, 2)
    steps = [("qa", 2)] * (inner == 4) + [("qb", 1 << k) for k in range(nb.bit_length() - 1)]
    sides = []
    for mask in range(1 << len(steps)):
        side_a, side_b, later = lax.rem(qa, inner), qb, jnp.int32(0)
        for k, (axis, bit) in enumerate(steps):
            if mask >> k & 1:
                there = lax.rem((qa if axis == "qa" else qb) // bit, 2)
                later += 1 - there
                side_a += (bit - 2 * bit * there) * (axis == "qa")
                side_b += (bit - 2 * bit * there) * (axis == "qb")
        sides.append((mask.bit_count(), later, side_a, side_b))

    def below(size, later):
        return later == 0

    def above(size, later):
        return later == size

    def tell(sem_of, low, high, chosen, both):
        for mask, (size, later, a, b) in enumerate(sides):
            for other in range(1 + both):

                @pl.when(chosen(size, later))
                def _():
                    skip = not mask and not other
                    bounds = (low + (skip and chosen is above), high - (skip and chosen is below))

                    def one(to_z, _):
                        to_a = to_z * inner + a + other * (1 - 2 * core)
                        pl.semaphore_signal(sem_of(size, to_z), inc=1, device_id=(to_a, b), device_id_type=MESH)

                    lax.fori_loop(*bounds, one, None)

    def send_levels(found):
        for mask, (_, later, a, b) in enumerate(sides):
            for other in range(2):
                ahead = z + found - later
                own_chip = 1 if not mask and not other else 0
                low = jnp.where(later < found, ahead, 0)
                high = jnp.where(later < found, jnp.minimum(ahead + 1, depth), jnp.where(later == found, z + 1 - own_chip, 0))

                def one(to_z, _):
                    to_a = to_z * inner + a + other * (1 - 2 * core)
                    pltpu.make_async_remote_copy(
                        src_ref=level.at[to_a * nb + b], dst_ref=levels.at[me],
                        send_sem=level_sem.at[1], recv_sem=level_sem.at[2],
                        device_id=(to_a, b), device_id_type=MESH,
                    ).start()

                lax.fori_loop(low, high, one, None)

    barrier = pltpu.get_barrier_semaphore()
    tell(lambda size, to_z: barrier, z, depth, above, True)
    nearer = sum(jnp.where(below(size, later), 1, 0) for size, later, _, _ in sides)
    pl.semaphore_wait(barrier, 2 * (z + 1) * nearer - 1)
    tell(lambda size, to_z: greet_sem.at[size + z - to_z - 1], 0, z + 1, below, False)
    load_level.wait()
    send_levels(0)
    pltpu.make_async_copy(level.at[me], levels.at[me], level_sem.at[0]).start()
    for found in range(1, len(steps) + depth):
        fresh = sum(
            jnp.where(above(size, later) & (found >= size) & (z + found - size < depth), 1, 0) for size, later, _, _ in sides
        )

        @pl.when(fresh > 0)
        def _():
            pl.semaphore_wait(greet_sem.at[found - 1], fresh)
            send_levels(found)

    rows_table[...] = sign_table(n * step)
    lanes_table[...] = sign_table(lanes)
    load_angle.wait()
    load_wave.wait()

    first = angle[0:1, :]

    @pl.loop(0, cuts)
    def _(cut):
        held = pl.ds(pl.multiple_of(cut * step, step), step)
        c, s = cos_sin(first * level[:, held, :].reshape(n * step, lanes), scales[0])
        x = wave[0, :, held, :].reshape(n * step, lanes)
        y = wave[1, :, held, :].reshape(n * step, lanes)
        done = mix_rows_lanes(rows_table[...], lanes_table[...], x * c + y * s, y * c - x * s)
        for part in range(2):
            mixed[cut, part] = done[part].reshape(n, step, lanes)

    for part in range(2):

        @pl.loop(0, n // group)
        def _(i):
            ds = pl.ds(i * group, group)
            send0[:, ds, part] = mix_lead(mixed[:, part, ds])

    @pl.loop(0, cuts)
    def _(cut):
        exchange(send0.at[cut], got0.at[cut], own_sem.at[0, cut], ssem.at[0, cut], rsem.at[0, cut])

    received(level, levels, level_sem.at[0], level_sem.at[2])
    second = angle[1:2, :]

    @pl.loop(0, n)
    def _(d):
        c, s = cos_sin(second * levels[d], scales[1])
        cosine[d] = c
        sine[d] = s

    @pl.loop(0, cuts)
    def _(cut):
        received(send0.at[cut], got0.at[cut], own_sem.at[0, cut], rsem.at[0, cut])
        held = pl.ds(pl.multiple_of(cut * step, step), step)
        x, y = mix_lead(got0[cut, :, 0]), mix_lead(got0[cut, :, 1])
        c, s = cosine[:, held, :], sine[:, held, :]
        x, y = (x * c + y * s).reshape(n * step, lanes), (y * c - x * s).reshape(n * step, lanes)
        done = mix_rows_lanes(rows_table[...], lanes_table[...], x, y)
        for part in range(2):
            send1[cut, :, part] = done[part].reshape(n, step, lanes)
        exchange(send1.at[cut], got1.at[cut], own_sem.at[1, cut], ssem.at[1, cut], rsem.at[1, cut])

    few = min(8, step)
    for cut in range(cuts):
        received(send1.at[cut], got1.at[cut], own_sem.at[1, cut], rsem.at[1, cut])
        last = cut == cuts - 1

        for part in range(2):
            for row in range(0, step, few):
                done = mix_lead(got1[cut, :, part, row : row + few])
                if not last:
                    mixed[cut, part, :, row : row + few] = done
                    continue
                parts = [mixed[k, part, :, row : row + few] for k in range(cut)] + [done]
                for k, value in enumerate(mix_list(parts)):
                    out_ref[part, :, k * step + row : k * step + row + few, :] = value

    left(level, level_sem.at[1])

    @pl.loop(0, cuts)
    def _(cut):
        left(send0.at[cut], ssem.at[0, cut])
        left(send1.at[cut], ssem.at[1, cut])


def put_out(state_ref, out_hbm, sem):
    copy = pltpu.make_async_copy(state_ref, out_hbm, sem)
    copy.start()
    copy.wait()


def far_first(na, nb):
    inner = min(na, 4)

    def rank(offset):
        ka, kb = offset
        high, aside, core = ka // inner, ka % inner // 2 + kb.bit_count(), ka % 2
        return high >= na // inner // 2, high, -aside, core

    return sorted([(ka, kb) for ka in range(na) for kb in range(nb) if ka or kb], key=rank)


STEP = 16
SPACE = 40 * 2**20


def body(wave_parts, level_table, phase_angles):
    na, nb = lax.axis_size("qa"), lax.axis_size("qb")
    n = na * nb
    _, blocks, rows, lanes = wave_parts.shape
    piece = blocks * rows // n
    step = min(STEP, piece)
    cuts = piece // step
    bits = (n * blocks * rows * lanes).bit_length() - 1
    scales = (2.0 ** -(bits // 2), 2.0 ** -(bits - bits // 2))
    hbm = pl.BlockSpec(memory_space=pltpu.HBM)
    f32 = jnp.float32
    flat = (2, n, piece, lanes)
    state = pltpu.VMEM((cuts, n, 2, step, lanes), f32)
    table = pltpu.VMEM((n, piece, lanes), f32)
    result = pl.pallas_call(
        functools.partial(kernel, na, nb, scales),
        out_shape=pltpu.VMEM(flat, f32),
        in_specs=[hbm, hbm, hbm],
        out_specs=pl.BlockSpec(memory_space=pltpu.VMEM),
        scratch_shapes=[
            pltpu.VMEM(flat, f32),
            table,
            pltpu.VMEM(phase_angles.shape, f32),
            pltpu.VMEM((n * step, n * step), jnp.bfloat16),
            pltpu.VMEM((lanes, lanes), jnp.bfloat16),
            pltpu.VMEM((cuts, 2, n, step, lanes), f32),
            state, state, state, state, table, table, table,
            pltpu.SemaphoreType.DMA((3,)),
            pltpu.SemaphoreType.DMA((2, cuts)),
            pltpu.SemaphoreType.DMA((2, cuts)),
            pltpu.SemaphoreType.DMA((2, cuts)),
            pltpu.SemaphoreType.DMA((3,)),
            pltpu.SemaphoreType.REGULAR((nb.bit_length() + na,)),
        ],
        compiler_params=pltpu.CompilerParams(
            collective_id=0, has_side_effects=True, vmem_limit_bytes=SPACE
        ),
    )(*(
        pltpu.with_memory_space_constraint(x, pltpu.HBM)
        for x in (wave_parts.reshape(flat), level_table.reshape(n, piece, lanes), phase_angles)
    ))
    result = pl.pallas_call(
        put_out,
        out_shape=jax.ShapeDtypeStruct(flat, f32),
        in_specs=[pl.BlockSpec(memory_space=pltpu.VMEM)],
        out_specs=hbm,
        scratch_shapes=[pltpu.SemaphoreType.DMA],
        compiler_params=pltpu.CompilerParams(vmem_limit_bytes=4 * 2**20),
    )(result)
    return result.reshape(wave_parts.shape)


def solution(mesh):
    in_specs = (P(None, ("qa", "qb"), None, None), P(("qa", "qb"), None, None), P())
    out_specs = P(None, ("qa", "qb"), None, None)
    return jax.shard_map(body, mesh=mesh, in_specs=in_specs, out_specs=out_specs, check_vma=False)
```

```python
import functools

import jax
import jax.numpy as jnp
import numpy as np
from jax import lax
from jax.experimental import pallas as pl
from jax.experimental.pallas import tpu as pltpu
from jax.sharding import PartitionSpec as P

MESH = pl.DeviceIdType.MESH
TURN_MOST = 2.5


def fit_even(function, degree):
    top = TURN_MOST**2
    nodes = (np.cos(np.pi * (np.arange(64) + 0.5) / 64) + 1) * top / 2
    fit = np.polynomial.chebyshev.Chebyshev.fit(nodes, function(np.sqrt(nodes)), degree, domain=[0, top])
    return [float(c) for c in fit.convert(kind=np.polynomial.Polynomial).coef]


COS = fit_even(np.cos, 6)
SIN = fit_even(lambda t: np.sin(t) / t, 5)


def horner(coefs, u, scale):
    total = jnp.float32(coefs[-1] * scale)
    for c in coefs[-2::-1]:
        total = total * u + jnp.float32(c * scale)
    return total


def cos_sin(turn, scale):
    u = turn * turn
    return horner(COS, u, scale), turn * horner(SIN, u, scale)


def sign_table(count):
    both = lax.broadcasted_iota(jnp.int32, (count, count), 0) & lax.broadcasted_iota(jnp.int32, (count, count), 1)
    shift = 1
    while shift < count.bit_length():
        shift *= 2
    while shift > 1:
        shift //= 2
        both = both ^ (both >> shift)
    return (1 - 2 * (both & 1)).astype(jnp.float32).astype(jnp.bfloat16)


def mix_lead(x):
    n = x.shape[0]
    half = 1
    while half < n:
        y = x.reshape((n // (2 * half), 2, half) + x.shape[1:])
        x = jnp.stack([y[:, 0] + y[:, 1], y[:, 0] - y[:, 1]], axis=1).reshape(x.shape)
        half *= 2
    return x


def mix_list(parts):
    half = 1
    while half < len(parts):
        mixed = list(parts)
        for k in range(len(parts)):
            if not k & half:
                mixed[k], mixed[k + half] = parts[k] + parts[k + half], parts[k] - parts[k + half]
        parts = mixed
        half *= 2
    return parts


def dot(a, b):
    return jnp.dot(a, b, preferred_element_type=jnp.float32)


def halves(x):
    hi = x.astype(jnp.bfloat16)
    return hi, (x - hi.astype(jnp.float32)).astype(jnp.bfloat16)


def mix_rows_lanes(rows, lanes, x, y):
    hi, lo = halves(jnp.concatenate([x, y], axis=1))
    both = dot(rows, hi) + dot(rows, lo)
    width = x.shape[1]
    out = []
    for part in (both[:, :width], both[:, width:]):
        hi, lo = halves(part)
        out.append(dot(hi, lanes) + dot(lo, lanes))
    return out


def kernel(
    na, nb, scales, wave_hbm, level_hbm, angle_hbm, got1, mixed_ref,
    wave, level, angle, rows_table, lanes_table, mixed, send0, got0, send1, levels, cosine, sine,
    load_sem, ssem, rsem, level_sem, greet_sem,
):
    n = na * nb
    cuts, _, _, step, lanes = send0.shape
    qa, qb = lax.axis_index("qa"), lax.axis_index("qb")
    me = qa * nb + qb
    group = 4

    def flips(q, count):
        found = [q]
        bit = 1
        while bit < count:
            change = bit - 2 * bit * lax.rem(q // bit, 2)
            found = found + [f + change for f in found]
            bit *= 2
        return found

    to_as, to_bs = flips(qa, na), flips(qb, nb)
    order = far_first(na, nb)
    peers = [(to_as[ka], to_bs[kb], to_as[ka] * nb + to_bs[kb]) for ka, kb in order]

    load_wave = pltpu.make_async_copy(wave_hbm, wave, load_sem.at[0])
    load_level = pltpu.make_async_copy(level_hbm, level, load_sem.at[1])
    load_angle = pltpu.make_async_copy(angle_hbm, angle, load_sem.at[2])
    load_level.start()
    load_angle.start()

    def exchange(source, target, sent, got):
        pltpu.make_async_copy(source.at[me], target.at[me], got).start()
        for to_a, to_b, to in peers:
            pltpu.make_async_remote_copy(
                src_ref=source.at[to], dst_ref=target.at[me], send_sem=sent, recv_sem=got,
                device_id=(to_a, to_b), device_id_type=MESH,
            ).start()

    def received(target, got):
        pltpu.make_async_copy(target, target, got).wait()

    def left(source, sent):
        rest = source.at[pl.ds(0, n - 1)]
        pltpu.make_async_copy(rest, rest, sent).wait()

    inner = min(na, 4)
    depth = na // inner
    z, core = qa // inner, lax.rem(qa, 2)
    steps = [("qa", 2)] * (inner == 4) + [("qb", 1 << k) for k in range(nb.bit_length() - 1)]
    sides = []
    for mask in range(1 << len(steps)):
        side_a, side_b, later = lax.rem(qa, inner), qb, jnp.int32(0)
        for k, (axis, bit) in enumerate(steps):
            if mask >> k & 1:
                there = lax.rem((qa if axis == "qa" else qb) // bit, 2)
                later += 1 - there
                side_a += (bit - 2 * bit * there) * (axis == "qa")
                side_b += (bit - 2 * bit * there) * (axis == "qb")
        sides.append((mask.bit_count(), later, side_a, side_b))

    def below(size, later):
        return later == 0

    def above(size, later):
        return later == size

    def tell(sem_of, low, high, chosen, both):
        for mask, (size, later, a, b) in enumerate(sides):
            for other in range(1 + both):

                @pl.when(chosen(size, later))
                def _():
                    skip = not mask and not other
                    bounds = (low + (not mask and not other), high)

                    def one(at, _):
                        to_z = at if chosen is above else z - at
                        to_a = to_z * inner + a + other * (1 - 2 * core)
                        pl.semaphore_signal(sem_of(size, to_z), inc=1, device_id=(to_a, b), device_id_type=MESH)

                    lax.fori_loop(*bounds, one, None)

    def send_levels(found):
        for mask, (_, later, a, b) in enumerate(sides):
            for other in range(2):
                ahead = z + found - later
                own_chip = 1 if not mask and not other else 0
                low = jnp.where(later < found, ahead, 0)
                high = jnp.where(later < found, jnp.minimum(ahead + 1, depth), jnp.where(later == found, z + 1 - own_chip, 0))

                def one(to_z, _):
                    to_a = to_z * inner + a + other * (1 - 2 * core)
                    pltpu.make_async_remote_copy(
                        src_ref=level.at[to_a * nb + b], dst_ref=levels.at[me],
                        send_sem=level_sem.at[0], recv_sem=level_sem.at[1],
                        device_id=(to_a, b), device_id_type=MESH,
                    ).start()

                lax.fori_loop(low, high, one, None)

    barrier = pltpu.get_barrier_semaphore()
    tell(lambda size, to_z: barrier, z, depth, above, True)
    nearer = sum(jnp.where(below(size, later), 1, 0) for size, later, _, _ in sides)
    pl.semaphore_wait(barrier, 2 * (z + 1) * nearer - 1)
    tell(lambda size, to_z: greet_sem.at[size + z - to_z - 1], 0, z + 1, below, False)
    load_level.wait()
    load_wave.start()
    send_levels(0)
    pltpu.make_async_copy(level.at[me], levels.at[me], level_sem.at[1]).start()
    for found in range(1, len(steps) + depth):
        fresh = sum(
            jnp.where(above(size, later) & (found >= size) & (z + found - size < depth), 1, 0) for size, later, _, _ in sides
        )

        @pl.when(fresh > 0)
        def _():
            pl.semaphore_wait(greet_sem.at[found - 1], fresh)
            send_levels(found)

    rows_table[...] = sign_table(n * step)
    lanes_table[...] = sign_table(lanes)
    load_angle.wait()
    load_wave.wait()

    first = angle[0:1, :]

    @pl.loop(0, cuts)
    def _(cut):
        held = pl.ds(pl.multiple_of(cut * step, step), step)
        c, s = cos_sin(first * level[:, held, :].reshape(n * step, lanes), scales[0])
        x = wave[0, :, held, :].reshape(n * step, lanes)
        y = wave[1, :, held, :].reshape(n * step, lanes)
        done = mix_rows_lanes(rows_table[...], lanes_table[...], x * c + y * s, y * c - x * s)
        for part in range(2):
            mixed[cut, part] = done[part].reshape(n, step, lanes)

    for part in range(2):

        @pl.loop(0, n // group)
        def _(i):
            ds = pl.ds(i * group, group)
            send0[:, ds, part] = mix_lead(mixed[:, part, ds])

    @pl.loop(0, cuts)
    def _(cut):
        exchange(send0.at[cut], got0.at[cut], ssem.at[0, cut], rsem.at[0, cut])

    received(levels, level_sem.at[1])
    second = angle[1:2, :]

    @pl.loop(0, n)
    def _(d):
        c, s = cos_sin(second * levels[d], scales[1])
        cosine[d] = c
        sine[d] = s

    @pl.loop(0, cuts)
    def _(cut):
        received(got0.at[cut], rsem.at[0, cut])
        held = pl.ds(pl.multiple_of(cut * step, step), step)
        x, y = mix_lead(got0[cut, :, 0]), mix_lead(got0[cut, :, 1])
        c, s = cosine[:, held, :], sine[:, held, :]
        x, y = (x * c + y * s).reshape(n * step, lanes), (y * c - x * s).reshape(n * step, lanes)
        done = mix_rows_lanes(rows_table[...], lanes_table[...], x, y)
        for part in range(2):
            send1[cut, :, part] = done[part].reshape(n, step, lanes)
        exchange(send1.at[cut], got1.at[cut], ssem.at[1, cut], rsem.at[1, cut])

    few = min(8, step)
    for cut in range(cuts):
        received(got1.at[cut], rsem.at[1, cut])
        if cut == cuts - 1:
            continue
        for part in range(2):
            for row in range(0, step, few):
                mixed_ref[cut, part, :, row : row + few] = mix_lead(got1[cut, :, part, row : row + few])

    left(level, level_sem.at[0])

    @pl.loop(0, cuts)
    def _(cut):
        left(send0.at[cut], ssem.at[0, cut])
        left(send1.at[cut], ssem.at[1, cut])


def put_out(got_ref, mixed_ref, out_hbm, out, sem):
    cuts, _, _, step, _ = mixed_ref.shape
    few = min(8, step)
    for row in range(0, step, few):
        for part in range(2):
            done = mix_lead(got_ref[cuts - 1, :, part, row : row + few])
            parts = [mixed_ref[k, part, :, row : row + few] for k in range(cuts - 1)] + [done]
            for k, value in enumerate(mix_list(parts)):
                out[part, :, k * step + row : k * step + row + few, :] = value
        for k in range(cuts):
            rows = pl.ds(k * step + row, few)
            pltpu.make_async_copy(out.at[:, :, rows], out_hbm.at[:, :, rows], sem).start()
    pltpu.make_async_copy(out, out_hbm, sem).wait()


def far_first(na, nb):
    inner = min(na, 4)

    def rank(offset):
        ka, kb = offset
        high, aside, core = ka // inner, ka % inner // 2 + kb.bit_count(), ka % 2
        return high >= na // inner // 2, high, -aside, core

    return sorted([(ka, kb) for ka in range(na) for kb in range(nb) if ka or kb], key=rank)


STEP = 16
SPACE = 40 * 2**20


def body(wave_parts, level_table, phase_angles):
    na, nb = lax.axis_size("qa"), lax.axis_size("qb")
    n = na * nb
    _, blocks, rows, lanes = wave_parts.shape
    piece = blocks * rows // n
    step = min(STEP, piece)
    cuts = piece // step
    bits = (n * blocks * rows * lanes).bit_length() - 1
    scales = (2.0 ** -(bits // 2), 2.0 ** -(bits - bits // 2))
    hbm = pl.BlockSpec(memory_space=pltpu.HBM)
    f32 = jnp.float32
    flat = (2, n, piece, lanes)
    state = pltpu.VMEM((cuts, n, 2, step, lanes), f32)
    table = pltpu.VMEM((n, piece, lanes), f32)
    result = pl.pallas_call(
        functools.partial(kernel, na, nb, scales),
        out_shape=(pltpu.VMEM(state.shape, f32), pltpu.VMEM((cuts, 2, n, step, lanes), f32)),
        in_specs=[hbm, hbm, hbm],
        out_specs=(pl.BlockSpec(memory_space=pltpu.VMEM),) * 2,
        scratch_shapes=[
            pltpu.VMEM(flat, f32),
            table,
            pltpu.VMEM(phase_angles.shape, f32),
            pltpu.VMEM((n * step, n * step), jnp.bfloat16),
            pltpu.VMEM((lanes, lanes), jnp.bfloat16),
            pltpu.VMEM((cuts, 2, n, step, lanes), f32),
            state, state, state, table, table, table,
            pltpu.SemaphoreType.DMA((3,)),
            pltpu.SemaphoreType.DMA((2, cuts)),
            pltpu.SemaphoreType.DMA((2, cuts)),
            pltpu.SemaphoreType.DMA((2,)),
            pltpu.SemaphoreType.REGULAR((nb.bit_length() + max(na // 4, 1),)),
        ],
        compiler_params=pltpu.CompilerParams(
            collective_id=0, has_side_effects=True, vmem_limit_bytes=SPACE
        ),
    )(*(
        pltpu.with_memory_space_constraint(x, pltpu.HBM)
        for x in (wave_parts.reshape(flat), level_table.reshape(n, piece, lanes), phase_angles)
    ))
    result = pl.pallas_call(
        put_out,
        out_shape=jax.ShapeDtypeStruct(flat, f32),
        in_specs=[pl.BlockSpec(memory_space=pltpu.VMEM)] * 2,
        out_specs=hbm,
        scratch_shapes=[pltpu.VMEM(flat, f32), pltpu.SemaphoreType.DMA],
        compiler_params=pltpu.CompilerParams(vmem_limit_bytes=8 * 2**20),
    )(*result)
    return result.reshape(wave_parts.shape)


def solution(mesh):
    in_specs = (P(None, ("qa", "qb"), None, None), P(("qa", "qb"), None, None), P())
    out_specs = P(None, ("qa", "qb"), None, None)
    return jax.shard_map(body, mesh=mesh, in_specs=in_specs, out_specs=out_specs, check_vma=False)
```

```python
import functools

import jax
import jax.numpy as jnp
import numpy as np
from jax import lax
from jax.experimental import pallas as pl
from jax.experimental.pallas import tpu as pltpu
from jax.sharding import PartitionSpec as P

MESH = pl.DeviceIdType.MESH
TURN_MOST = 2.5


def fit_even(function, degree):
    top = TURN_MOST**2
    nodes = (np.cos(np.pi * (np.arange(64) + 0.5) / 64) + 1) * top / 2
    fit = np.polynomial.chebyshev.Chebyshev.fit(nodes, function(np.sqrt(nodes)), degree, domain=[0, top])
    return [float(c) for c in fit.convert(kind=np.polynomial.Polynomial).coef]


COS = fit_even(np.cos, 6)
SIN = fit_even(lambda t: np.sin(t) / t, 5)


def horner(coefs, u, scale):
    total = jnp.float32(coefs[-1] * scale)
    for c in coefs[-2::-1]:
        total = total * u + jnp.float32(c * scale)
    return total


def cos_sin(turn, scale):
    u = turn * turn
    return horner(COS, u, scale), turn * horner(SIN, u, scale)


def sign_table(count):
    both = lax.broadcasted_iota(jnp.int32, (count, count), 0) & lax.broadcasted_iota(jnp.int32, (count, count), 1)
    shift = 1
    while shift < count.bit_length():
        shift *= 2
    while shift > 1:
        shift //= 2
        both = both ^ (both >> shift)
    return (1 - 2 * (both & 1)).astype(jnp.float32).astype(jnp.bfloat16)


def mix_lead(x):
    n = x.shape[0]
    half = 1
    while half < n:
        y = x.reshape((n // (2 * half), 2, half) + x.shape[1:])
        x = jnp.stack([y[:, 0] + y[:, 1], y[:, 0] - y[:, 1]], axis=1).reshape(x.shape)
        half *= 2
    return x


def mix_list(parts):
    half = 1
    while half < len(parts):
        mixed = list(parts)
        for k in range(len(parts)):
            if not k & half:
                mixed[k], mixed[k + half] = parts[k] + parts[k + half], parts[k] - parts[k + half]
        parts = mixed
        half *= 2
    return parts


def dot(a, b):
    return jnp.dot(a, b, preferred_element_type=jnp.float32)


def halves(x):
    hi = x.astype(jnp.bfloat16)
    return hi, (x - hi.astype(jnp.float32)).astype(jnp.bfloat16)


def mix_rows_lanes(rows, lanes, x, y):
    hi, lo = halves(jnp.concatenate([x, y], axis=1))
    both = dot(rows, hi) + dot(rows, lo)
    width = x.shape[1]
    out = []
    for part in (both[:, :width], both[:, width:]):
        hi, lo = halves(part)
        out.append(dot(hi, lanes) + dot(lo, lanes))
    return out


def kernel(
    na, nb, scales, wave_hbm, level_hbm, angle_hbm, got1, mixed_ref,
    wave, level, angle, rows_table, lanes_table, mixed, send0, got0, send1, levels, cosine, sine,
    load_sem, ssem, rsem, level_sem, greet_sem,
):
    n = na * nb
    cuts, _, _, step, lanes = send0.shape
    qa, qb = lax.axis_index("qa"), lax.axis_index("qb")
    me = qa * nb + qb
    group = 4

    def flips(q, count):
        found = [q]
        bit = 1
        while bit < count:
            change = bit - 2 * bit * lax.rem(q // bit, 2)
            found = found + [f + change for f in found]
            bit *= 2
        return found

    to_as, to_bs = flips(qa, na), flips(qb, nb)
    aside = lax.rem(qa // 2, 2) == 1

    def place(ka, kb):
        to_a, to_b = to_as[ka], to_bs[kb]
        if min(na, 4) == 4 and kb < 2 and ka // 2 % 2 != kb:
            to_a, to_b = jnp.where(aside, to_a, to_as[ka ^ 2]), jnp.where(aside, to_b, to_bs[kb ^ 1])
        if ka > 1 or kb:
            to_a += 1 - ka % 2 - lax.rem(to_a, 2)
        return to_a, to_b, to_a * nb + to_b

    peers = [place(ka, kb) for ka, kb in far_first(na, nb)]

    load_wave = pltpu.make_async_copy(wave_hbm, wave, load_sem.at[0])
    load_level = pltpu.make_async_copy(level_hbm, level, load_sem.at[1])
    load_angle = pltpu.make_async_copy(angle_hbm, angle, load_sem.at[2])
    load_level.start()
    load_angle.start()

    def exchange(source, target, sent, got):
        pltpu.make_async_copy(source.at[me], target.at[me], got).start()
        for to_a, to_b, to in peers:
            pltpu.make_async_remote_copy(
                src_ref=source.at[to], dst_ref=target.at[me], send_sem=sent, recv_sem=got,
                device_id=(to_a, to_b), device_id_type=MESH,
            ).start()

    def received(target, got):
        pltpu.make_async_copy(target, target, got).wait()

    def left(source, sent):
        rest = source.at[pl.ds(0, n - 1)]
        pltpu.make_async_copy(rest, rest, sent).wait()

    inner = min(na, 4)
    depth = na // inner
    z, core = qa // inner, lax.rem(qa, 2)
    steps = [("qa", 2)] * (inner == 4) + [("qb", 1 << k) for k in range(nb.bit_length() - 1)]
    sides = []
    for mask in range(1 << len(steps)):
        side_a, side_b, later = lax.rem(qa, inner), qb, jnp.int32(0)
        for k, (axis, bit) in enumerate(steps):
            if mask >> k & 1:
                there = lax.rem((qa if axis == "qa" else qb) // bit, 2)
                later += 1 - there
                side_a += (bit - 2 * bit * there) * (axis == "qa")
                side_b += (bit - 2 * bit * there) * (axis == "qb")
        sides.append((mask.bit_count(), later, side_a, side_b))

    def below(size, later):
        return later == 0

    def above(size, later):
        return later == size

    def tell(sem_of, low, high, chosen, both):
        for mask, (size, later, a, b) in enumerate(sides):
            for other in range(1 + both):

                @pl.when(chosen(size, later))
                def _():
                    skip = not mask and not other
                    bounds = (low + (not mask and not other), high)

                    def one(at, _):
                        to_z = at if chosen is above else z - at
                        to_a = to_z * inner + a + other * (1 - 2 * core)
                        pl.semaphore_signal(sem_of(size, to_z), inc=1, device_id=(to_a, b), device_id_type=MESH)

                    lax.fori_loop(*bounds, one, None)

    def send_levels(found):
        for mask, (_, later, a, b) in enumerate(sides):
            for other in range(2):
                ahead = z + found - later
                own_chip = 1 if not mask and not other else 0
                low = jnp.where(later < found, ahead, 0)
                high = jnp.where(later < found, jnp.minimum(ahead + 1, depth), jnp.where(later == found, z + 1 - own_chip, 0))

                def one(to_z, _):
                    to_a = to_z * inner + a + other * (1 - 2 * core)
                    pltpu.make_async_remote_copy(
                        src_ref=level.at[to_a * nb + b], dst_ref=levels.at[me],
                        send_sem=level_sem.at[0], recv_sem=level_sem.at[1],
                        device_id=(to_a, b), device_id_type=MESH,
                    ).start()

                lax.fori_loop(low, high, one, None)

    barrier = pltpu.get_barrier_semaphore()
    tell(lambda size, to_z: barrier, z, depth, above, True)
    nearer = sum(jnp.where(below(size, later), 1, 0) for size, later, _, _ in sides)
    pl.semaphore_wait(barrier, 2 * (z + 1) * nearer - 1)
    tell(lambda size, to_z: greet_sem.at[size + z - to_z - 1], 0, z + 1, below, False)
    load_level.wait()
    load_wave.start()
    send_levels(0)
    pltpu.make_async_copy(level.at[me], levels.at[me], level_sem.at[1]).start()
    for found in range(1, len(steps) + depth):
        fresh = sum(
            jnp.where(above(size, later) & (found >= size) & (z + found - size < depth), 1, 0) for size, later, _, _ in sides
        )

        @pl.when(fresh > 0)
        def _():
            pl.semaphore_wait(greet_sem.at[found - 1], fresh)
            send_levels(found)

    rows_table[...] = sign_table(n * step)
    lanes_table[...] = sign_table(lanes)
    load_angle.wait()
    load_wave.wait()

    first = angle[0:1, :]

    @pl.loop(0, cuts)
    def _(cut):
        held = pl.ds(pl.multiple_of(cut * step, step), step)
        c, s = cos_sin(first * level[:, held, :].reshape(n * step, lanes), scales[0])
        x = wave[0, :, held, :].reshape(n * step, lanes)
        y = wave[1, :, held, :].reshape(n * step, lanes)
        done = mix_rows_lanes(rows_table[...], lanes_table[...], x * c + y * s, y * c - x * s)
        for part in range(2):
            mixed[cut, part] = done[part].reshape(n, step, lanes)

    for part in range(2):

        @pl.loop(0, n // group)
        def _(i):
            ds = pl.ds(i * group, group)
            send0[:, ds, part] = mix_lead(mixed[:, part, ds])

    @pl.loop(0, cuts)
    def _(cut):
        exchange(send0.at[cut], got0.at[cut], ssem.at[0, cut], rsem.at[0, cut])

    received(levels, level_sem.at[1])
    second = angle[1:2, :]

    @pl.loop(0, n)
    def _(d):
        c, s = cos_sin(second * levels[d], scales[1])
        cosine[d] = c
        sine[d] = s

    @pl.loop(0, cuts)
    def _(cut):
        received(got0.at[cut], rsem.at[0, cut])
        held = pl.ds(pl.multiple_of(cut * step, step), step)
        x, y = mix_lead(got0[cut, :, 0]), mix_lead(got0[cut, :, 1])
        c, s = cosine[:, held, :], sine[:, held, :]
        x, y = (x * c + y * s).reshape(n * step, lanes), (y * c - x * s).reshape(n * step, lanes)
        done = mix_rows_lanes(rows_table[...], lanes_table[...], x, y)
        for part in range(2):
            send1[cut, :, part] = done[part].reshape(n, step, lanes)
        exchange(send1.at[cut], got1.at[cut], ssem.at[1, cut], rsem.at[1, cut])

    few = min(8, step)
    for cut in range(cuts):
        received(got1.at[cut], rsem.at[1, cut])
        if cut == cuts - 1:
            continue
        for part in range(2):
            for row in range(0, step, few):
                mixed_ref[cut, part, :, row : row + few] = mix_lead(got1[cut, :, part, row : row + few])

    left(level, level_sem.at[0])

    @pl.loop(0, cuts)
    def _(cut):
        left(send0.at[cut], ssem.at[0, cut])
        left(send1.at[cut], ssem.at[1, cut])


def put_out(got_ref, mixed_ref, out_hbm, out, sem):
    cuts, _, _, step, _ = mixed_ref.shape
    few = min(8, step)
    for row in range(0, step, few):
        for part in range(2):
            done = mix_lead(got_ref[cuts - 1, :, part, row : row + few])
            parts = [mixed_ref[k, part, :, row : row + few] for k in range(cuts - 1)] + [done]
            for k, value in enumerate(mix_list(parts)):
                rows = pl.ds(k * step + row, few)
                out[part, :, rows, :] = value
                pltpu.make_async_copy(out.at[part, :, rows], out_hbm.at[part, :, rows], sem).start()
    pltpu.make_async_copy(out, out_hbm, sem).wait()


def far_first(na, nb):
    inner = min(na, 4)

    def rank(offset):
        ka, kb = offset
        high, aside, core = ka // inner, ka % inner // 2 + kb.bit_count(), ka % 2
        return high >= na // inner // 2, high, -aside, ka % inner < 2, core

    return sorted([(ka, kb) for ka in range(na) for kb in range(nb) if ka or kb], key=rank)


STEP = 16
SPACE = 40 * 2**20


def body(wave_parts, level_table, phase_angles):
    na, nb = lax.axis_size("qa"), lax.axis_size("qb")
    n = na * nb
    _, blocks, rows, lanes = wave_parts.shape
    piece = blocks * rows // n
    step = min(STEP, piece)
    cuts = piece // step
    bits = (n * blocks * rows * lanes).bit_length() - 1
    scales = (2.0 ** -(bits // 2), 2.0 ** -(bits - bits // 2))
    hbm = pl.BlockSpec(memory_space=pltpu.HBM)
    f32 = jnp.float32
    flat = (2, n, piece, lanes)
    state = pltpu.VMEM((cuts, n, 2, step, lanes), f32)
    table = pltpu.VMEM((n, piece, lanes), f32)
    result = pl.pallas_call(
        functools.partial(kernel, na, nb, scales),
        out_shape=(pltpu.VMEM(state.shape, f32), pltpu.VMEM((cuts, 2, n, step, lanes), f32)),
        in_specs=[hbm, hbm, hbm],
        out_specs=(pl.BlockSpec(memory_space=pltpu.VMEM),) * 2,
        scratch_shapes=[
            pltpu.VMEM(flat, f32),
            table,
            pltpu.VMEM(phase_angles.shape, f32),
            pltpu.VMEM((n * step, n * step), jnp.bfloat16),
            pltpu.VMEM((lanes, lanes), jnp.bfloat16),
            pltpu.VMEM((cuts, 2, n, step, lanes), f32),
            state, state, state, table, table, table,
            pltpu.SemaphoreType.DMA((3,)),
            pltpu.SemaphoreType.DMA((2, cuts)),
            pltpu.SemaphoreType.DMA((2, cuts)),
            pltpu.SemaphoreType.DMA((2,)),
            pltpu.SemaphoreType.REGULAR((nb.bit_length() + max(na // 4, 1),)),
        ],
        compiler_params=pltpu.CompilerParams(
            collective_id=0, has_side_effects=True, vmem_limit_bytes=SPACE
        ),
    )(*(
        pltpu.with_memory_space_constraint(x, pltpu.HBM)
        for x in (wave_parts.reshape(flat), level_table.reshape(n, piece, lanes), phase_angles)
    ))
    result = pl.pallas_call(
        put_out,
        out_shape=jax.ShapeDtypeStruct(flat, f32),
        in_specs=[pl.BlockSpec(memory_space=pltpu.VMEM)] * 2,
        out_specs=hbm,
        scratch_shapes=[pltpu.VMEM(flat, f32), pltpu.SemaphoreType.DMA],
        compiler_params=pltpu.CompilerParams(vmem_limit_bytes=8 * 2**20),
    )(*result)
    return result.reshape(wave_parts.shape)


def solution(mesh):
    in_specs = (P(None, ("qa", "qb"), None, None), P(("qa", "qb"), None, None), P())
    out_specs = P(None, ("qa", "qb"), None, None)
    return jax.shard_map(body, mesh=mesh, in_specs=in_specs, out_specs=out_specs, check_vma=False)
```

```python
import functools

import jax
import jax.numpy as jnp
import numpy as np
from jax import lax
from jax.experimental import pallas as pl
from jax.experimental.pallas import tpu as pltpu
from jax.sharding import PartitionSpec as P

MESH = pl.DeviceIdType.MESH
TURN_MOST = 2.5


def fit_even(function, degree):
    top = TURN_MOST**2
    nodes = (np.cos(np.pi * (np.arange(64) + 0.5) / 64) + 1) * top / 2
    fit = np.polynomial.chebyshev.Chebyshev.fit(nodes, function(np.sqrt(nodes)), degree, domain=[0, top])
    return [float(c) for c in fit.convert(kind=np.polynomial.Polynomial).coef]


COS = fit_even(np.cos, 6)
SIN = fit_even(lambda t: np.sin(t) / t, 5)


def horner(coefs, u, scale):
    total = jnp.float32(coefs[-1] * scale)
    for c in coefs[-2::-1]:
        total = total * u + jnp.float32(c * scale)
    return total


def cos_sin(turn, scale):
    u = turn * turn
    return horner(COS, u, scale), turn * horner(SIN, u, scale)


def sign_table(count):
    both = lax.broadcasted_iota(jnp.int32, (count, count), 0) & lax.broadcasted_iota(jnp.int32, (count, count), 1)
    shift = 1
    while shift < count.bit_length():
        shift *= 2
    while shift > 1:
        shift //= 2
        both = both ^ (both >> shift)
    return (1 - 2 * (both & 1)).astype(jnp.float32).astype(jnp.bfloat16)


def mix_lead(x):
    n = x.shape[0]
    half = 1
    while half < n:
        y = x.reshape((n // (2 * half), 2, half) + x.shape[1:])
        x = jnp.stack([y[:, 0] + y[:, 1], y[:, 0] - y[:, 1]], axis=1).reshape(x.shape)
        half *= 2
    return x


def mix_list(parts):
    half = 1
    while half < len(parts):
        mixed = list(parts)
        for k in range(len(parts)):
            if not k & half:
                mixed[k], mixed[k + half] = parts[k] + parts[k + half], parts[k] - parts[k + half]
        parts = mixed
        half *= 2
    return parts


def dot(a, b):
    return jnp.dot(a, b, preferred_element_type=jnp.float32)


def halves(x):
    hi = x.astype(jnp.bfloat16)
    return hi, (x - hi.astype(jnp.float32)).astype(jnp.bfloat16)


def mix_rows_lanes(rows, lanes, x, y):
    hi, lo = halves(jnp.concatenate([x, y], axis=1))
    both = dot(rows, hi) + dot(rows, lo)
    width = x.shape[1]
    out = []
    for part in (both[:, :width], both[:, width:]):
        hi, lo = halves(part)
        out.append(dot(hi, lanes) + dot(lo, lanes))
    return out


def kernel(
    na, nb, scales, wave_hbm, level_hbm, angle_hbm, got1,
    wave, level, angle, rows_table, lanes_table, mixed, send0, got0, send1, levels, cosine, sine,
    load_sem, ssem, rsem, level_sem, greet_sem,
):
    n = na * nb
    cuts, _, _, step, lanes = send0.shape
    qa, qb = lax.axis_index("qa"), lax.axis_index("qb")
    me = qa * nb + qb
    group = 4

    def flips(q, count):
        found = [q]
        bit = 1
        while bit < count:
            change = bit - 2 * bit * lax.rem(q // bit, 2)
            found = found + [f + change for f in found]
            bit *= 2
        return found

    to_as, to_bs = flips(qa, na), flips(qb, nb)
    aside = lax.rem(qa // 2, 2) == 1

    def place(ka, kb):
        to_a, to_b = to_as[ka], to_bs[kb]
        if min(na, 4) == 4 and kb < 2 and ka // 2 % 2 != kb:
            to_a, to_b = jnp.where(aside, to_a, to_as[ka ^ 2]), jnp.where(aside, to_b, to_bs[kb ^ 1])
        if ka > 1 or kb:
            to_a += 1 - ka % 2 - lax.rem(to_a, 2)
        return to_a, to_b, to_a * nb + to_b

    peers = [place(ka, kb) for ka, kb in far_first(na, nb)]

    load_wave = pltpu.make_async_copy(wave_hbm, wave, load_sem.at[0])
    load_level = pltpu.make_async_copy(level_hbm, level, load_sem.at[1])
    load_angle = pltpu.make_async_copy(angle_hbm, angle, load_sem.at[2])
    load_level.start()
    load_angle.start()

    def exchange(source, target, sent, got, chosen=slice(None)):
        if chosen.stop is None:
            pltpu.make_async_copy(source.at[me], target.at[me], got).start()
        for to_a, to_b, to in peers[chosen]:
            pltpu.make_async_remote_copy(
                src_ref=source.at[to], dst_ref=target.at[me], send_sem=sent, recv_sem=got,
                device_id=(to_a, to_b), device_id_type=MESH,
            ).start()

    def received(target, got):
        pltpu.make_async_copy(target, target, got).wait()

    def left(source, sent):
        rest = source.at[pl.ds(0, n - 1)]
        pltpu.make_async_copy(rest, rest, sent).wait()

    inner = min(na, 4)
    depth = na // inner
    z, core = qa // inner, lax.rem(qa, 2)
    steps = [("qa", 2)] * (inner == 4) + [("qb", 1 << k) for k in range(nb.bit_length() - 1)]
    sides = []
    for mask in range(1 << len(steps)):
        side_a, side_b, later = lax.rem(qa, inner), qb, jnp.int32(0)
        for k, (axis, bit) in enumerate(steps):
            if mask >> k & 1:
                there = lax.rem((qa if axis == "qa" else qb) // bit, 2)
                later += 1 - there
                side_a += (bit - 2 * bit * there) * (axis == "qa")
                side_b += (bit - 2 * bit * there) * (axis == "qb")
        sides.append((mask.bit_count(), later, side_a, side_b))

    def below(size, later):
        return later == 0

    def above(size, later):
        return later == size

    def tell(sem_of, low, high, chosen, both):
        for mask, (size, later, a, b) in enumerate(sides):
            for other in range(1 + both):

                @pl.when(chosen(size, later))
                def _():
                    skip = not mask and not other
                    bounds = (low + (not mask and not other), high)

                    def one(at, _):
                        to_z = at if chosen is above else z - at
                        to_a = to_z * inner + a + other * (1 - 2 * core)
                        pl.semaphore_signal(sem_of(size, to_z), inc=1, device_id=(to_a, b), device_id_type=MESH)

                    lax.fori_loop(*bounds, one, None)

    def send_levels(found):
        for mask, (_, later, a, b) in enumerate(sides):
            for other in range(2):
                ahead = z + found - later
                own_chip = 1 if not mask and not other else 0
                low = jnp.where(later < found, ahead, 0)
                high = jnp.where(later < found, jnp.minimum(ahead + 1, depth), jnp.where(later == found, z + 1 - own_chip, 0))

                def one(to_z, _):
                    to_a = to_z * inner + a + other * (1 - 2 * core)
                    pltpu.make_async_remote_copy(
                        src_ref=level.at[to_a * nb + b], dst_ref=levels.at[me],
                        send_sem=level_sem.at[0], recv_sem=level_sem.at[1],
                        device_id=(to_a, b), device_id_type=MESH,
                    ).start()

                lax.fori_loop(low, high, one, None)

    barrier = pltpu.get_barrier_semaphore()
    tell(lambda size, to_z: barrier, z, depth, above, True)
    nearer = sum(jnp.where(below(size, later), 1, 0) for size, later, _, _ in sides)
    pl.semaphore_wait(barrier, 2 * (z + 1) * nearer - 1)
    tell(lambda size, to_z: greet_sem.at[size + z - to_z - 1], 0, z + 1, below, False)
    load_level.wait()
    load_wave.start()
    send_levels(0)
    pltpu.make_async_copy(level.at[me], levels.at[me], level_sem.at[1]).start()
    for found in range(1, len(steps) + depth):
        fresh = sum(
            jnp.where(above(size, later) & (found >= size) & (z + found - size < depth), 1, 0) for size, later, _, _ in sides
        )

        @pl.when(fresh > 0)
        def _():
            pl.semaphore_wait(greet_sem.at[found - 1], fresh)
            send_levels(found)

    rows_table[...] = sign_table(n * step)
    lanes_table[...] = sign_table(lanes)
    load_angle.wait()
    load_wave.wait()

    first = angle[0:1, :]

    @pl.loop(0, cuts)
    def _(cut):
        held = pl.ds(pl.multiple_of(cut * step, step), step)
        c, s = cos_sin(first * level[:, held, :].reshape(n * step, lanes), scales[0])
        x = wave[0, :, held, :].reshape(n * step, lanes)
        y = wave[1, :, held, :].reshape(n * step, lanes)
        done = mix_rows_lanes(rows_table[...], lanes_table[...], x * c + y * s, y * c - x * s)
        for part in range(2):
            mixed[cut, part] = done[part].reshape(n, step, lanes)

    for part in range(2):

        @pl.loop(0, n // group)
        def _(i):
            ds = pl.ds(i * group, group)
            send0[:, ds, part] = mix_lead(mixed[:, part, ds])

    @pl.loop(0, cuts)
    def _(cut):
        exchange(send0.at[cut], got0.at[cut], ssem.at[0, cut], rsem.at[0, cut])

    received(levels, level_sem.at[1])
    second = angle[1:2, :]

    @pl.loop(0, n)
    def _(d):
        c, s = cos_sin(second * levels[d], scales[1])
        cosine[d] = c
        sine[d] = s

    @pl.loop(0, cuts)
    def _(cut):
        received(got0.at[cut], rsem.at[0, cut])
        held = pl.ds(pl.multiple_of(cut * step, step), step)
        x, y = mix_lead(got0[cut, :, 0]), mix_lead(got0[cut, :, 1])
        c, s = cosine[:, held, :], sine[:, held, :]
        x, y = (x * c + y * s).reshape(n * step, lanes), (y * c - x * s).reshape(n * step, lanes)
        done = mix_rows_lanes(rows_table[...], lanes_table[...], x, y)
        for part in range(2):
            send1[cut, :, part] = done[part].reshape(n, step, lanes)
        pltpu.make_async_copy(send1.at[cut, me], got1.at[cut, me], rsem.at[1, cut]).start()
        exchange(send1.at[cut], got1.at[cut], ssem.at[1, cut], rsem.at[1, cut], slice(0, n - 1 - LATE))

    @pl.loop(0, cuts)
    def _(cut):
        exchange(send1.at[cut], got1.at[cut], ssem.at[1, cut], rsem.at[1, cut], slice(n - 1 - LATE, n))

    @pl.loop(0, cuts)
    def _(cut):
        received(got1.at[cut], rsem.at[1, cut])

    left(level, level_sem.at[0])

    @pl.loop(0, cuts)
    def _(cut):
        left(send0.at[cut], ssem.at[0, cut])
        left(send1.at[cut], ssem.at[1, cut])


def put_out(got_ref, out_hbm, out, sem):
    cuts, _, _, step, _ = got_ref.shape
    few = min(8, step)
    for row in range(0, step, few):
        for part in range(2):
            parts = [mix_lead(got_ref[k, :, part, row : row + few]) for k in range(cuts)]
            for k, value in enumerate(mix_list(parts)):
                rows = pl.ds(k * step + row, few)
                out[part, :, rows, :] = value
                pltpu.make_async_copy(out.at[part, :, rows], out_hbm.at[part, :, rows], sem).start()
    pltpu.make_async_copy(out, out_hbm, sem).wait()


def far_first(na, nb):
    inner = min(na, 4)

    def rank(offset):
        ka, kb = offset
        high, aside, core = ka // inner, ka % inner // 2 + kb.bit_count(), ka % 2
        return high >= na // inner // 2, high, -aside, ka % inner < 2, core

    return sorted([(ka, kb) for ka in range(na) for kb in range(nb) if ka or kb], key=rank)


STEP = 16
LATE = 2
SPACE = 40 * 2**20


def body(wave_parts, level_table, phase_angles):
    na, nb = lax.axis_size("qa"), lax.axis_size("qb")
    n = na * nb
    _, blocks, rows, lanes = wave_parts.shape
    piece = blocks * rows // n
    step = min(STEP, piece)
    cuts = piece // step
    bits = (n * blocks * rows * lanes).bit_length() - 1
    scales = (2.0 ** -(bits // 2), 2.0 ** -(bits - bits // 2))
    hbm = pl.BlockSpec(memory_space=pltpu.HBM)
    f32 = jnp.float32
    flat = (2, n, piece, lanes)
    state = pltpu.VMEM((cuts, n, 2, step, lanes), f32)
    table = pltpu.VMEM((n, piece, lanes), f32)
    result = pl.pallas_call(
        functools.partial(kernel, na, nb, scales),
        out_shape=pltpu.VMEM(state.shape, f32),
        in_specs=[hbm, hbm, hbm],
        out_specs=pl.BlockSpec(memory_space=pltpu.VMEM),
        scratch_shapes=[
            pltpu.VMEM(flat, f32),
            table,
            pltpu.VMEM(phase_angles.shape, f32),
            pltpu.VMEM((n * step, n * step), jnp.bfloat16),
            pltpu.VMEM((lanes, lanes), jnp.bfloat16),
            pltpu.VMEM((cuts, 2, n, step, lanes), f32),
            state, state, state, table, table, table,
            pltpu.SemaphoreType.DMA((3,)),
            pltpu.SemaphoreType.DMA((2, cuts)),
            pltpu.SemaphoreType.DMA((2, cuts)),
            pltpu.SemaphoreType.DMA((2,)),
            pltpu.SemaphoreType.REGULAR((nb.bit_length() + max(na // 4, 1),)),
        ],
        compiler_params=pltpu.CompilerParams(
            collective_id=0, has_side_effects=True, vmem_limit_bytes=SPACE
        ),
    )(*(
        pltpu.with_memory_space_constraint(x, pltpu.HBM)
        for x in (wave_parts.reshape(flat), level_table.reshape(n, piece, lanes), phase_angles)
    ))
    result = pl.pallas_call(
        put_out,
        out_shape=jax.ShapeDtypeStruct(flat, f32),
        in_specs=[pl.BlockSpec(memory_space=pltpu.VMEM)],
        out_specs=hbm,
        scratch_shapes=[pltpu.VMEM(flat, f32), pltpu.SemaphoreType.DMA],
        compiler_params=pltpu.CompilerParams(vmem_limit_bytes=8 * 2**20),
    )(result)
    return result.reshape(wave_parts.shape)


def solution(mesh):
    in_specs = (P(None, ("qa", "qb"), None, None), P(("qa", "qb"), None, None), P())
    out_specs = P(None, ("qa", "qb"), None, None)
    return jax.shard_map(body, mesh=mesh, in_specs=in_specs, out_specs=out_specs, check_vma=False)
```

```python
import functools

import jax
import jax.numpy as jnp
import numpy as np
from jax import lax
from jax.experimental import pallas as pl
from jax.experimental.pallas import tpu as pltpu
from jax.sharding import PartitionSpec as P

MESH = pl.DeviceIdType.MESH
TURN_MOST = 2.5


def fit_even(function, degree):
    top = TURN_MOST**2
    nodes = (np.cos(np.pi * (np.arange(64) + 0.5) / 64) + 1) * top / 2
    fit = np.polynomial.chebyshev.Chebyshev.fit(nodes, function(np.sqrt(nodes)), degree, domain=[0, top])
    return [float(c) for c in fit.convert(kind=np.polynomial.Polynomial).coef]


COS = fit_even(np.cos, 6)
SIN = fit_even(lambda t: np.sin(t) / t, 5)


def horner(coefs, u, scale):
    total = jnp.float32(coefs[-1] * scale)
    for c in coefs[-2::-1]:
        total = total * u + jnp.float32(c * scale)
    return total


def cos_sin(turn, scale):
    u = turn * turn
    return horner(COS, u, scale), turn * horner(SIN, u, scale)


def sign_table(count):
    both = lax.broadcasted_iota(jnp.int32, (count, count), 0) & lax.broadcasted_iota(jnp.int32, (count, count), 1)
    shift = 1
    while shift < count.bit_length():
        shift *= 2
    while shift > 1:
        shift //= 2
        both = both ^ (both >> shift)
    return (1 - 2 * (both & 1)).astype(jnp.float32).astype(jnp.bfloat16)


def mix_lead(x):
    n = x.shape[0]
    half = 1
    while half < n:
        y = x.reshape((n // (2 * half), 2, half) + x.shape[1:])
        x = jnp.stack([y[:, 0] + y[:, 1], y[:, 0] - y[:, 1]], axis=1).reshape(x.shape)
        half *= 2
    return x


def mix_list(parts):
    half = 1
    while half < len(parts):
        mixed = list(parts)
        for k in range(len(parts)):
            if not k & half:
                mixed[k], mixed[k + half] = parts[k] + parts[k + half], parts[k] - parts[k + half]
        parts = mixed
        half *= 2
    return parts


def dot(a, b):
    return jnp.dot(a, b, preferred_element_type=jnp.float32)


def halves(x):
    hi = x.astype(jnp.bfloat16)
    return hi, (x - hi.astype(jnp.float32)).astype(jnp.bfloat16)


def mix_rows_lanes(rows, lanes, x, y):
    hi, lo = halves(jnp.concatenate([x, y], axis=1))
    both = dot(rows, hi) + dot(rows, lo)
    width = x.shape[1]
    out = []
    for part in (both[:, :width], both[:, width:]):
        hi, lo = halves(part)
        out.append(dot(hi, lanes) + dot(lo, lanes))
    return out


def kernel(
    na, nb, scales, wave_hbm, level_hbm, angle_hbm, got1,
    wave, level, angle, rows_table, lanes_table, mixed, sends, got0, levels, cosine, sine,
    load_sem, ssem, rsem, level_sem, greet_sem,
):
    n = na * nb
    _, cuts, _, _, step, lanes = sends.shape
    send0, send1 = sends.at[0], sends.at[1]
    qa, qb = lax.axis_index("qa"), lax.axis_index("qb")
    me = qa * nb + qb
    group = 4

    def flips(q, count):
        found = [q]
        bit = 1
        while bit < count:
            change = bit - 2 * bit * lax.rem(q // bit, 2)
            found = found + [f + change for f in found]
            bit *= 2
        return found

    to_as, to_bs = flips(qa, na), flips(qb, nb)
    aside = lax.rem(qa // 2, 2) == 1

    def place(ka, kb):
        to_a, to_b = to_as[ka], to_bs[kb]
        if min(na, 4) == 4 and kb < 2 and ka // 2 % 2 != kb:
            to_a, to_b = jnp.where(aside, to_a, to_as[ka ^ 2]), jnp.where(aside, to_b, to_bs[kb ^ 1])
        if ka > 1 or kb:
            to_a += 1 - ka % 2 - lax.rem(to_a, 2)
        return to_a, to_b, to_a * nb + to_b

    peers = [place(ka, kb) for ka, kb in far_first(na, nb)]

    load_wave = pltpu.make_async_copy(wave_hbm, wave, load_sem.at[0])
    load_level = pltpu.make_async_copy(level_hbm, level, load_sem.at[1])
    load_angle = pltpu.make_async_copy(angle_hbm, angle, load_sem.at[2])
    load_level.start()
    load_angle.start()

    def exchange(source, target, sent, got, chosen=slice(None)):
        if chosen.stop is None:
            pltpu.make_async_copy(source.at[me], target.at[me], got).start()
        for to_a, to_b, to in peers[chosen]:
            pltpu.make_async_remote_copy(
                src_ref=source.at[to], dst_ref=target.at[me], send_sem=sent, recv_sem=got,
                device_id=(to_a, to_b), device_id_type=MESH,
            ).start()

    def received(target, got):
        pltpu.make_async_copy(target, target, got).wait()

    def left(source, sent):
        rest = source.at[pl.ds(0, n - 1)]
        pltpu.make_async_copy(rest, rest, sent).wait()

    inner = min(na, 4)
    depth = na // inner
    z, core = qa // inner, lax.rem(qa, 2)
    steps = [("qa", 2)] * (inner == 4) + [("qb", 1 << k) for k in range(nb.bit_length() - 1)]
    sides = []
    for mask in range(1 << len(steps)):
        side_a, side_b, later = lax.rem(qa, inner), qb, jnp.int32(0)
        for k, (axis, bit) in enumerate(steps):
            if mask >> k & 1:
                there = lax.rem((qa if axis == "qa" else qb) // bit, 2)
                later += 1 - there
                side_a += (bit - 2 * bit * there) * (axis == "qa")
                side_b += (bit - 2 * bit * there) * (axis == "qb")
        sides.append((mask.bit_count(), later, side_a, side_b))

    def below(size, later):
        return later == 0

    def above(size, later):
        return later == size

    def tell(sem_of, low, high, chosen, both):
        for mask, (size, later, a, b) in enumerate(sides):
            for other in range(1 + both):

                @pl.when(chosen(size, later))
                def _():
                    skip = not mask and not other
                    bounds = (low + (not mask and not other), high)

                    def one(at, _):
                        to_z = at if chosen is above else z - at
                        to_a = to_z * inner + a + other * (1 - 2 * core)
                        pl.semaphore_signal(sem_of(size, to_z), inc=1, device_id=(to_a, b), device_id_type=MESH)

                    lax.fori_loop(*bounds, one, None)

    def send_levels(found):
        for mask, (_, later, a, b) in enumerate(sides):
            for other in range(2):
                ahead = z + found - later
                own_chip = 1 if not mask and not other else 0
                low = jnp.where(later < found, ahead, 0)
                high = jnp.where(later < found, jnp.minimum(ahead + 1, depth), jnp.where(later == found, z + 1 - own_chip, 0))

                def one(to_z, _):
                    to_a = to_z * inner + a + other * (1 - 2 * core)
                    pltpu.make_async_remote_copy(
                        src_ref=level.at[to_a * nb + b], dst_ref=levels.at[me],
                        send_sem=level_sem.at[0], recv_sem=level_sem.at[1],
                        device_id=(to_a, b), device_id_type=MESH,
                    ).start()

                lax.fori_loop(low, high, one, None)

    barrier = pltpu.get_barrier_semaphore()
    tell(lambda size, to_z: barrier, z, depth, above, True)
    nearer = sum(jnp.where(below(size, later), 1, 0) for size, later, _, _ in sides)
    pl.semaphore_wait(barrier, 2 * (z + 1) * nearer - 1)
    tell(lambda size, to_z: greet_sem.at[size + z - to_z - 1], 0, z + 1, below, False)
    load_level.wait()
    load_wave.start()
    send_levels(0)
    pltpu.make_async_copy(level.at[me], levels.at[me], level_sem.at[1]).start()
    for found in range(1, len(steps) + depth):
        fresh = sum(
            jnp.where(above(size, later) & (found >= size) & (z + found - size < depth), 1, 0) for size, later, _, _ in sides
        )

        @pl.when(fresh > 0)
        def _():
            pl.semaphore_wait(greet_sem.at[found - 1], fresh)
            send_levels(found)

    rows_table[...] = sign_table(n * step)
    lanes_table[...] = sign_table(lanes)
    load_angle.wait()
    load_wave.wait()

    first = angle[0:1, :]

    @pl.loop(0, cuts)
    def _(cut):
        held = pl.ds(pl.multiple_of(cut * step, step), step)
        c, s = cos_sin(first * level[:, held, :].reshape(n * step, lanes), scales[0])
        x = wave[0, :, held, :].reshape(n * step, lanes)
        y = wave[1, :, held, :].reshape(n * step, lanes)
        done = mix_rows_lanes(rows_table[...], lanes_table[...], x * c + y * s, y * c - x * s)
        for part in range(2):
            mixed[cut, part] = done[part].reshape(n, step, lanes)

    for part in range(2):

        @pl.loop(0, n // group)
        def _(i):
            ds = pl.ds(i * group, group)
            send0[:, ds, part] = mix_lead(mixed[:, part, ds])

    @pl.loop(0, cuts)
    def _(cut):
        exchange(send0.at[cut], got0.at[cut], ssem, rsem.at[0, cut])

    received(levels, level_sem.at[1])
    second = angle[1:2, :]

    @pl.loop(0, n)
    def _(d):
        c, s = cos_sin(second * levels[d], scales[1])
        cosine[d] = c
        sine[d] = s

    @pl.loop(0, cuts)
    def _(cut):
        received(got0.at[cut], rsem.at[0, cut])
        held = pl.ds(pl.multiple_of(cut * step, step), step)
        x, y = mix_lead(got0[cut, :, 0]), mix_lead(got0[cut, :, 1])
        c, s = cosine[:, held, :], sine[:, held, :]
        x, y = (x * c + y * s).reshape(n * step, lanes), (y * c - x * s).reshape(n * step, lanes)
        done = mix_rows_lanes(rows_table[...], lanes_table[...], x, y)
        for part in range(2):
            send1[cut, :, part] = done[part].reshape(n, step, lanes)
        pltpu.make_async_copy(send1.at[cut, me], got1.at[cut, me], rsem.at[1, cut]).start()
        exchange(send1.at[cut], got1.at[cut], ssem, rsem.at[1, cut], slice(0, n - 1 - LATE))

    @pl.loop(0, cuts)
    def _(cut):
        exchange(send1.at[cut], got1.at[cut], ssem, rsem.at[1, cut], slice(n - 1 - LATE, n))

    @pl.loop(0, cuts)
    def _(cut):
        received(got1.at[cut], rsem.at[1, cut])

    left(level, level_sem.at[0])
    rest = sends.at[:, :, pl.ds(0, n - 1)]
    pltpu.make_async_copy(rest, rest, ssem).wait()


def put_out(got_ref, out_hbm, out, sem):
    cuts, _, _, step, _ = got_ref.shape
    few = min(8, step)
    for row in range(0, step, few):
        for part in range(2):
            parts = [mix_lead(got_ref[k, :, part, row : row + few]) for k in range(cuts)]
            for k, value in enumerate(mix_list(parts)):
                rows = pl.ds(k * step + row, few)
                out[part, :, rows, :] = value
                pltpu.make_async_copy(out.at[part, :, rows], out_hbm.at[part, :, rows], sem).start()
    pltpu.make_async_copy(out, out_hbm, sem).wait()


def far_first(na, nb):
    inner = min(na, 4)

    def rank(offset):
        ka, kb = offset
        high, aside, core = ka // inner, ka % inner // 2 + kb.bit_count(), ka % 2
        crossing, last = high >= na // inner // 2, high == na // inner - 1
        weight = 20 * crossing + 5 * last - aside + (ka % inner < 2) + (high == 1) + 4 * (last and not aside)
        return weight, high, aside

    return sorted([(ka, kb) for ka in range(na) for kb in range(nb) if ka or kb], key=rank)


STEP = 16
LATE = 2
SPACE = 40 * 2**20


def body(wave_parts, level_table, phase_angles):
    na, nb = lax.axis_size("qa"), lax.axis_size("qb")
    n = na * nb
    _, blocks, rows, lanes = wave_parts.shape
    piece = blocks * rows // n
    step = min(STEP, piece)
    cuts = piece // step
    bits = (n * blocks * rows * lanes).bit_length() - 1
    scales = (2.0 ** -(bits // 2), 2.0 ** -(bits - bits // 2))
    hbm = pl.BlockSpec(memory_space=pltpu.HBM)
    f32 = jnp.float32
    flat = (2, n, piece, lanes)
    state = pltpu.VMEM((cuts, n, 2, step, lanes), f32)
    table = pltpu.VMEM((n, piece, lanes), f32)
    result = pl.pallas_call(
        functools.partial(kernel, na, nb, scales),
        out_shape=pltpu.VMEM(state.shape, f32),
        in_specs=[hbm, hbm, hbm],
        out_specs=pl.BlockSpec(memory_space=pltpu.VMEM),
        scratch_shapes=[
            pltpu.VMEM(flat, f32),
            table,
            pltpu.VMEM(phase_angles.shape, f32),
            pltpu.VMEM((n * step, n * step), jnp.bfloat16),
            pltpu.VMEM((lanes, lanes), jnp.bfloat16),
            pltpu.VMEM((cuts, 2, n, step, lanes), f32),
            pltpu.VMEM((2, *state.shape), f32), state, table, table, table,
            pltpu.SemaphoreType.DMA((3,)),
            pltpu.SemaphoreType.DMA,
            pltpu.SemaphoreType.DMA((2, cuts)),
            pltpu.SemaphoreType.DMA((2,)),
            pltpu.SemaphoreType.REGULAR((nb.bit_length() + max(na // 4, 1),)),
        ],
        compiler_params=pltpu.CompilerParams(
            collective_id=0, has_side_effects=True, vmem_limit_bytes=SPACE
        ),
    )(*(
        pltpu.with_memory_space_constraint(x, pltpu.HBM)
        for x in (wave_parts.reshape(flat), level_table.reshape(n, piece, lanes), phase_angles)
    ))
    result = pl.pallas_call(
        put_out,
        out_shape=jax.ShapeDtypeStruct(flat, f32),
        in_specs=[pl.BlockSpec(memory_space=pltpu.VMEM)],
        out_specs=hbm,
        scratch_shapes=[pltpu.VMEM(flat, f32), pltpu.SemaphoreType.DMA],
        compiler_params=pltpu.CompilerParams(vmem_limit_bytes=8 * 2**20),
    )(result)
    return result.reshape(wave_parts.shape)


def solution(mesh):
    in_specs = (P(None, ("qa", "qb"), None, None), P(("qa", "qb"), None, None), P())
    out_specs = P(None, ("qa", "qb"), None, None)
    return jax.shard_map(body, mesh=mesh, in_specs=in_specs, out_specs=out_specs, check_vma=False)
```

```python
import functools

import jax
import jax.numpy as jnp
import numpy as np
from jax import lax
from jax.experimental import pallas as pl
from jax.experimental.pallas import tpu as pltpu
from jax.sharding import PartitionSpec as P

MESH = pl.DeviceIdType.MESH
TURN_MOST = 2.5


def fit_even(function, degree):
    top = TURN_MOST**2
    nodes = (np.cos(np.pi * (np.arange(64) + 0.5) / 64) + 1) * top / 2
    fit = np.polynomial.chebyshev.Chebyshev.fit(nodes, function(np.sqrt(nodes)), degree, domain=[0, top])
    return [float(c) for c in fit.convert(kind=np.polynomial.Polynomial).coef]


COS = fit_even(np.cos, 6)
SIN = fit_even(lambda t: np.sin(t) / t, 5)


def horner(coefs, u, scale):
    total = jnp.float32(coefs[-1] * scale)
    for c in coefs[-2::-1]:
        total = total * u + jnp.float32(c * scale)
    return total


def cos_sin(turn, scale):
    u = turn * turn
    return horner(COS, u, scale), turn * horner(SIN, u, scale)


def sign_table(count):
    both = lax.broadcasted_iota(jnp.int32, (count, count), 0) & lax.broadcasted_iota(jnp.int32, (count, count), 1)
    shift = 1
    while shift < count.bit_length():
        shift *= 2
    while shift > 1:
        shift //= 2
        both = both ^ (both >> shift)
    return (1 - 2 * (both & 1)).astype(jnp.float32).astype(jnp.bfloat16)


def mix_lead(x):
    n = x.shape[0]
    half = 1
    while half < n:
        y = x.reshape((n // (2 * half), 2, half) + x.shape[1:])
        x = jnp.stack([y[:, 0] + y[:, 1], y[:, 0] - y[:, 1]], axis=1).reshape(x.shape)
        half *= 2
    return x


def mix_list(parts):
    half = 1
    while half < len(parts):
        mixed = list(parts)
        for k in range(len(parts)):
            if not k & half:
                mixed[k], mixed[k + half] = parts[k] + parts[k + half], parts[k] - parts[k + half]
        parts = mixed
        half *= 2
    return parts


def dot(a, b):
    return jnp.dot(a, b, preferred_element_type=jnp.float32)


def halves(x):
    hi = x.astype(jnp.bfloat16)
    return hi, (x - hi.astype(jnp.float32)).astype(jnp.bfloat16)


def mix_rows_lanes(rows, lanes, x, y):
    hi, lo = halves(jnp.concatenate([x, y], axis=1))
    both = dot(rows, hi) + dot(rows, lo)
    width = x.shape[1]
    out = []
    for part in (both[:, :width], both[:, width:]):
        hi, lo = halves(part)
        out.append(dot(hi, lanes) + dot(lo, lanes))
    return out


def kernel(
    na, nb, scales, wave_hbm, level_hbm, angle_hbm, got1,
    wave, level, angle, rows_table, lanes_table, mixed, sends, got0, levels, cosine, sine,
    load_sem, ssem, rsem, level_sem, greet_sem,
):
    n = na * nb
    _, cuts, _, _, step, lanes = sends.shape
    send0, send1 = sends.at[0], sends.at[1]
    qa, qb = lax.axis_index("qa"), lax.axis_index("qb")
    me = qa * nb + qb
    group = 4

    def flips(q, count):
        found = [q]
        bit = 1
        while bit < count:
            change = bit - 2 * bit * lax.rem(q // bit, 2)
            found = found + [f + change for f in found]
            bit *= 2
        return found

    to_as, to_bs = flips(qa, na), flips(qb, nb)
    aside = lax.rem(qa // 2, 2) == 1

    def place(ka, kb):
        to_a, to_b = to_as[ka], to_bs[kb]
        if min(na, 4) == 4 and kb < 2 and ka // 2 % 2 != kb:
            to_a, to_b = jnp.where(aside, to_a, to_as[ka ^ 2]), jnp.where(aside, to_b, to_bs[kb ^ 1])
        if ka > 1 or kb:
            to_a += 1 - ka % 2 - lax.rem(to_a, 2)
        return to_a, to_b, to_a * nb + to_b

    peers = [place(ka, kb) for ka, kb in far_first(na, nb)]

    load_wave = pltpu.make_async_copy(wave_hbm, wave, load_sem.at[0])
    load_level = pltpu.make_async_copy(level_hbm, level, load_sem.at[1])
    load_angle = pltpu.make_async_copy(angle_hbm, angle, load_sem.at[2])
    load_level.start()
    load_angle.start()

    def exchange(source, target, sent, got, chosen=slice(None)):
        if chosen.stop is None:
            pltpu.make_async_copy(source.at[me], target.at[me], got).start()
        for to_a, to_b, to in peers[chosen]:
            pltpu.make_async_remote_copy(
                src_ref=source.at[to], dst_ref=target.at[me], send_sem=sent, recv_sem=got,
                device_id=(to_a, to_b), device_id_type=MESH,
            ).start()

    def received(target, got):
        pltpu.make_async_copy(target, target, got).wait()

    def left(source, sent):
        rest = source.at[pl.ds(0, n - 1)]
        pltpu.make_async_copy(rest, rest, sent).wait()

    inner = min(na, 4)
    depth = na // inner
    z, core = qa // inner, lax.rem(qa, 2)
    steps = [("qa", 2)] * (inner == 4) + [("qb", 1 << k) for k in range(nb.bit_length() - 1)]
    sides = []
    for mask in range(1 << len(steps)):
        side_a, side_b, later = lax.rem(qa, inner), qb, jnp.int32(0)
        for k, (axis, bit) in enumerate(steps):
            if mask >> k & 1:
                there = lax.rem((qa if axis == "qa" else qb) // bit, 2)
                later += 1 - there
                side_a += (bit - 2 * bit * there) * (axis == "qa")
                side_b += (bit - 2 * bit * there) * (axis == "qb")
        sides.append((mask.bit_count(), later, side_a, side_b))

    def below(size, later):
        return later == 0

    def above(size, later):
        return later == size

    def tell(sem_of, low, high, chosen, both):
        for mask, (size, later, a, b) in enumerate(sides):
            for other in range(1 + both):

                @pl.when(chosen(size, later))
                def _():
                    skip = not mask and not other
                    bounds = (low + (not mask and not other), high)

                    def one(at, _):
                        to_z = at if chosen is above else z - at
                        to_a = to_z * inner + a + other * (1 - 2 * core)
                        pl.semaphore_signal(sem_of(size, to_z), inc=1, device_id=(to_a, b), device_id_type=MESH)

                    lax.fori_loop(*bounds, one, None)

    def send_levels(found):
        for mask, (_, later, a, b) in enumerate(sides):
            for other in range(2):
                ahead = z + found - later
                own_chip = 1 if not mask and not other else 0
                low = jnp.where(later < found, ahead, 0)
                high = jnp.where(later < found, jnp.minimum(ahead + 1, depth), jnp.where(later == found, z + 1 - own_chip, 0))

                def one(to_z, _):
                    to_a = to_z * inner + a + other * (1 - 2 * core)
                    pltpu.make_async_remote_copy(
                        src_ref=level.at[to_a * nb + b], dst_ref=levels.at[me],
                        send_sem=level_sem.at[0], recv_sem=level_sem.at[1],
                        device_id=(to_a, b), device_id_type=MESH,
                    ).start()

                lax.fori_loop(low, high, one, None)

    barrier = pltpu.get_barrier_semaphore()
    tell(lambda size, to_z: barrier, z, depth, above, True)
    nearer = sum(jnp.where(below(size, later), 1, 0) for size, later, _, _ in sides)
    pl.semaphore_wait(barrier, 2 * (z + 1) * nearer - 1)
    tell(lambda size, to_z: greet_sem.at[size + z - to_z - 1], 0, z + 1, below, False)
    load_level.wait()
    load_wave.start()
    send_levels(0)
    pltpu.make_async_copy(level.at[me], levels.at[me], level_sem.at[1]).start()
    for found in range(1, len(steps) + depth):
        fresh = sum(
            jnp.where(above(size, later) & (found >= size) & (z + found - size < depth), 1, 0) for size, later, _, _ in sides
        )

        @pl.when(fresh > 0)
        def _():
            pl.semaphore_wait(greet_sem.at[found - 1], fresh)
            send_levels(found)

    rows_table[...] = sign_table(n * step)
    lanes_table[...] = sign_table(lanes)
    load_angle.wait()
    load_wave.wait()

    first = angle[0:1, :]

    @pl.loop(0, cuts)
    def _(cut):
        held = pl.ds(pl.multiple_of(cut * step, step), step)
        c, s = cos_sin(first * level[:, held, :].reshape(n * step, lanes), scales[0])
        x = wave[0, :, held, :].reshape(n * step, lanes)
        y = wave[1, :, held, :].reshape(n * step, lanes)
        done = mix_rows_lanes(rows_table[...], lanes_table[...], x * c + y * s, y * c - x * s)
        for part in range(2):
            mixed[cut, part] = done[part].reshape(n, step, lanes)

    for part in range(2):

        @pl.loop(0, n // group)
        def _(i):
            ds = pl.ds(i * group, group)
            send0[:, ds, part] = mix_lead(mixed[:, part, ds])

    @pl.loop(0, cuts)
    def _(cut):
        exchange(send0.at[cut], got0.at[cut], ssem, rsem.at[0, cut])

    received(levels, level_sem.at[1])
    second = angle[1:2, :]

    @pl.loop(0, n)
    def _(d):
        c, s = cos_sin(second * levels[d], scales[1])
        cosine[d] = c
        sine[d] = s

    @pl.loop(0, cuts)
    def _(cut):
        received(got0.at[cut], rsem.at[0, cut])
        held = pl.ds(pl.multiple_of(cut * step, step), step)
        x, y = mix_lead(got0[cut, :, 0]), mix_lead(got0[cut, :, 1])
        c, s = cosine[:, held, :], sine[:, held, :]
        x, y = (x * c + y * s).reshape(n * step, lanes), (y * c - x * s).reshape(n * step, lanes)
        done = mix_rows_lanes(rows_table[...], lanes_table[...], x, y)
        for part in range(2):
            send1[cut, :, part] = done[part].reshape(n, step, lanes)
        pltpu.make_async_copy(send1.at[cut, me], got1.at[cut, me], rsem.at[1, cut]).start()
        exchange(send1.at[cut], got1.at[cut], ssem, rsem.at[1, cut], slice(0, n - 1 - LATE))

    @pl.loop(0, cuts)
    def _(cut):
        exchange(send1.at[cut], got1.at[cut], ssem, rsem.at[1, cut], slice(n - 1 - LATE, n))

    @pl.loop(0, cuts)
    def _(cut):
        received(got1.at[cut], rsem.at[1, cut])

    left(level, level_sem.at[0])
    rest = sends.at[:, :, pl.ds(0, n - 1)]
    pltpu.make_async_copy(rest, rest, ssem).wait()


def put_out(got_ref, out_hbm, out, sem):
    cuts, _, _, step, _ = got_ref.shape
    few = min(8, step)
    for part in range(2):
        for row in range(0, step, few):
            parts = [mix_lead(got_ref[k, :, part, row : row + few]) for k in range(cuts)]
            for k, value in enumerate(mix_list(parts)):
                rows = pl.ds(k * step + row, few)
                out[part, :, rows, :] = value
                pltpu.make_async_copy(out.at[part, :, rows], out_hbm.at[part, :, rows], sem).start()
    pltpu.make_async_copy(out, out_hbm, sem).wait()


def far_first(na, nb):
    inner = min(na, 4)

    def rank(offset):
        ka, kb = offset
        high, aside, core = ka // inner, ka % inner // 2 + kb.bit_count(), ka % 2
        crossing, last = high >= na // inner // 2, high == na // inner - 1
        weight = 20 * crossing + 5 * last - aside + (ka % inner < 2) + (high == 1) + 4 * (last and not aside)
        return weight, high, aside

    return sorted([(ka, kb) for ka in range(na) for kb in range(nb) if ka or kb], key=rank)


STEP = 16
LATE = 2
SPACE = 40 * 2**20


def body(wave_parts, level_table, phase_angles):
    na, nb = lax.axis_size("qa"), lax.axis_size("qb")
    n = na * nb
    _, blocks, rows, lanes = wave_parts.shape
    piece = blocks * rows // n
    step = min(STEP, piece)
    cuts = piece // step
    bits = (n * blocks * rows * lanes).bit_length() - 1
    scales = (2.0 ** -(bits // 2), 2.0 ** -(bits - bits // 2))
    hbm = pl.BlockSpec(memory_space=pltpu.HBM)
    f32 = jnp.float32
    flat = (2, n, piece, lanes)
    state = pltpu.VMEM((cuts, n, 2, step, lanes), f32)
    table = pltpu.VMEM((n, piece, lanes), f32)
    result = pl.pallas_call(
        functools.partial(kernel, na, nb, scales),
        out_shape=pltpu.VMEM(state.shape, f32),
        in_specs=[hbm, hbm, hbm],
        out_specs=pl.BlockSpec(memory_space=pltpu.VMEM),
        scratch_shapes=[
            pltpu.VMEM(flat, f32),
            table,
            pltpu.VMEM(phase_angles.shape, f32),
            pltpu.VMEM((n * step, n * step), jnp.bfloat16),
            pltpu.VMEM((lanes, lanes), jnp.bfloat16),
            pltpu.VMEM((cuts, 2, n, step, lanes), f32),
            pltpu.VMEM((2, *state.shape), f32), state, table, table, table,
            pltpu.SemaphoreType.DMA((3,)),
            pltpu.SemaphoreType.DMA,
            pltpu.SemaphoreType.DMA((2, cuts)),
            pltpu.SemaphoreType.DMA((2,)),
            pltpu.SemaphoreType.REGULAR((nb.bit_length() + max(na // 4, 1),)),
        ],
        compiler_params=pltpu.CompilerParams(
            collective_id=0, has_side_effects=True, vmem_limit_bytes=SPACE
        ),
    )(*(
        pltpu.with_memory_space_constraint(x, pltpu.HBM)
        for x in (wave_parts.reshape(flat), level_table.reshape(n, piece, lanes), phase_angles)
    ))
    result = pl.pallas_call(
        put_out,
        out_shape=jax.ShapeDtypeStruct(flat, f32),
        in_specs=[pl.BlockSpec(memory_space=pltpu.VMEM)],
        out_specs=hbm,
        scratch_shapes=[pltpu.VMEM(flat, f32), pltpu.SemaphoreType.DMA],
        compiler_params=pltpu.CompilerParams(vmem_limit_bytes=8 * 2**20),
    )(result)
    return result.reshape(wave_parts.shape)


def solution(mesh):
    in_specs = (P(None, ("qa", "qb"), None, None), P(("qa", "qb"), None, None), P())
    out_specs = P(None, ("qa", "qb"), None, None)
    return jax.shard_map(body, mesh=mesh, in_specs=in_specs, out_specs=out_specs, check_vma=False)
```
